128 devices in a mesh: data: 1, dap: 128 (over z, y, x, core).
Axes of the slice: x: 4, y: 4, z: 4, core: 2. Of those that a mesh axis runs over, the one named last changes fastest.
Arguments:
- pair_act: float32 [1024, 1024, 128], P(('data', 'dap'))
- pair_mask: int32 [1024, 1024], P(('data', 'dap'))
- msa_act: bfloat16 [64, 1024, 256], P(None, ('data', 'dap'))
- opm_norm: float32 [2, 256], replicated
- opm_proj: bfloat16 [256, 64], replicated
- opm_out: bfloat16 [1024, 128], replicated
- opm_bias: float32 [128], replicated
- tri_norm: float32 [2, 2, 128], replicated
- tri_proj: bfloat16 [2, 128, 512], replicated
- tri_gate: bfloat16 [2, 128, 128], replicated
- tri_xnorm: float32 [2, 2, 128], replicated
- tri_out: bfloat16 [2, 128, 128], replicated
Outputs:
- output: float32 [1024, 1024, 128], P(('data', 'dap'))
All inputs are finite; a program needn't handle non-finite values.
Results may differ from the reference program's by a relative error of at most 0.0030018.
Values are sent between devices in bfloat16 or wider.
A program may use at most 1 GiB of HBM per device.

```python
import jax
import jax.numpy as jnp
from jax import lax

RESIDUES = 1024
PAIR_DIM = 128
TRI_DIM = 128
MSA_DIM = 256
OPM_DIM = 32
MSA_DEPTH = 64
ROW_BLOCK = 32
NUM_BLOCKS = RESIDUES // ROW_BLOCK
LN_EPS = 1e-5


def layer_norm(values, norm_scale, norm_shift):
    row_mean = jnp.mean(values, axis=-1, keepdims=True)
    centered = values - row_mean
    row_var = jnp.mean(centered * centered, axis=-1, keepdims=True)
    return (centered * lax.rsqrt(row_var + LN_EPS) * norm_scale + norm_shift).astype(jnp.bfloat16)


def outer_product_mean(msa_act, opm_norm, opm_proj, opm_out, opm_bias):
    msa_norm = layer_norm(msa_act.astype(jnp.float32), opm_norm[0], opm_norm[1])
    proj_all = jnp.dot(msa_norm.reshape(MSA_DEPTH * RESIDUES, MSA_DIM), opm_proj, preferred_element_type=jnp.float32)
    proj_all = proj_all.astype(jnp.bfloat16).reshape(MSA_DEPTH, RESIDUES, 2 * OPM_DIM)
    left_proj = proj_all[:, :, :OPM_DIM].astype(jnp.float32)
    right_proj = proj_all[:, :, OPM_DIM:].astype(jnp.float32)
    left_blocks = jnp.moveaxis(left_proj.reshape(MSA_DEPTH, NUM_BLOCKS, ROW_BLOCK, OPM_DIM), 1, 0)

    def block_update(left_blk):
        outer_prod = jnp.einsum("sip,sjq->ijpq", left_blk, right_proj) / MSA_DEPTH
        outer_flat = outer_prod.astype(jnp.bfloat16).reshape(ROW_BLOCK * RESIDUES, OPM_DIM * OPM_DIM)
        return jnp.dot(outer_flat, opm_out, preferred_element_type=jnp.float32).reshape(ROW_BLOCK, RESIDUES, PAIR_DIM)

    opm_update = lax.map(block_update, left_blocks).reshape(RESIDUES, RESIDUES, PAIR_DIM)
    return opm_update + opm_bias


def triangle_update(pair_act, mask_f, norm_pair, w_proj, w_gate, norm_mix, w_out, incoming):
    pair_blocks = pair_act.reshape(NUM_BLOCKS, ROW_BLOCK, RESIDUES, PAIR_DIM)
    mask_blocks = mask_f.reshape(NUM_BLOCKS, ROW_BLOCK, RESIDUES, 1)

    def project(blk_args):
        pair_blk, mask_blk = blk_args
        pair_norm = layer_norm(pair_blk, norm_pair[0], norm_pair[1])
        proj_all = jnp.dot(pair_norm.reshape(ROW_BLOCK * RESIDUES, PAIR_DIM), w_proj, preferred_element_type=jnp.float32)
        proj_all = proj_all.reshape(ROW_BLOCK, RESIDUES, 4 * TRI_DIM)
        left_act = mask_blk * jax.nn.sigmoid(proj_all[:, :, TRI_DIM:2 * TRI_DIM]) * proj_all[:, :, :TRI_DIM]
        right_act = mask_blk * jax.nn.sigmoid(proj_all[:, :, 3 * TRI_DIM:]) * proj_all[:, :, 2 * TRI_DIM:3 * TRI_DIM]
        return left_act.astype(jnp.bfloat16), right_act.astype(jnp.bfloat16)

    left_all, right_all = lax.map(project, (pair_blocks, mask_blocks))
    left_all = left_all.reshape(RESIDUES, RESIDUES, TRI_DIM)
    right_all = right_all.reshape(RESIDUES, RESIDUES, TRI_DIM)
    if incoming:
        left_all = jnp.swapaxes(left_all, 0, 1)
        right_all = jnp.swapaxes(right_all, 0, 1)
    right_wide = right_all.astype(jnp.float32)
    left_blocks = left_all.reshape(NUM_BLOCKS, ROW_BLOCK, RESIDUES, TRI_DIM)

    def combine(blk_args):
        pair_blk, left_blk = blk_args
        mixed_act = jnp.einsum("ikc,jkc->ijc", left_blk.astype(jnp.float32), right_wide).astype(jnp.bfloat16)
        mixed_norm = layer_norm(mixed_act.astype(jnp.float32), norm_mix[0], norm_mix[1])
        update = jnp.dot(mixed_norm.reshape(ROW_BLOCK * RESIDUES, TRI_DIM), w_out, preferred_element_type=jnp.float32)
        pair_norm = layer_norm(pair_blk, norm_pair[0], norm_pair[1])
        gate_act = jax.nn.sigmoid(jnp.dot(pair_norm.reshape(ROW_BLOCK * RESIDUES, PAIR_DIM), w_gate, preferred_element_type=jnp.float32))
        return pair_blk + (gate_act * update).reshape(ROW_BLOCK, RESIDUES, PAIR_DIM)

    return lax.map(combine, (pair_blocks, left_blocks)).reshape(RESIDUES, RESIDUES, PAIR_DIM)


def setup_inputs(seed: int = 0, part: int = 0) -> dict:
    part_keys = jax.random.split(jax.random.fold_in(jax.random.key(seed), part), 5)
    shared_keys = jax.random.split(jax.random.key(seed + 1), 12)

    def scaled_normal(key_w, shape_w, fan_in):
        return (jax.random.normal(key_w, shape_w, jnp.float32) * fan_in ** -0.5).astype(jnp.bfloat16)

    pair_act = jax.random.normal(part_keys[0], (RESIDUES, RESIDUES, PAIR_DIM), jnp.float32)
    valid_len = jax.random.randint(part_keys[1], (), RESIDUES - RESIDUES // 8, RESIDUES - RESIDUES // 32 + 1)
    positions = jnp.arange(RESIDUES)
    in_range = positions < valid_len
    kept_entries = jax.random.randint(part_keys[2], (RESIDUES, RESIDUES), 0, 32) != 0
    pair_mask = (in_range[:, None] & in_range[None, :] & kept_entries).astype(jnp.int32)
    profile = jax.random.normal(part_keys[3], (RESIDUES, MSA_DIM), jnp.float32)
    msa_noise = jax.random.normal(part_keys[4], (MSA_DEPTH, RESIDUES, MSA_DIM), jnp.float32)
    msa_act = (profile[None] + 0.75 * msa_noise).astype(jnp.bfloat16)
    opm_norm = jnp.stack([1.0 + 0.3 * jax.random.normal(shared_keys[0], (MSA_DIM,), jnp.float32), 0.3 * jax.random.normal(shared_keys[1], (MSA_DIM,), jnp.float32)])
    opm_proj = scaled_normal(shared_keys[2], (MSA_DIM, 2 * OPM_DIM), MSA_DIM)
    opm_out = scaled_normal(shared_keys[3], (OPM_DIM * OPM_DIM, PAIR_DIM), OPM_DIM * OPM_DIM)
    opm_bias = 0.5 * jax.random.normal(shared_keys[4], (PAIR_DIM,), jnp.float32)
    tri_norm = jnp.concatenate([1.0 + 0.3 * jax.random.normal(shared_keys[5], (2, 1, PAIR_DIM), jnp.float32), 0.3 * jax.random.normal(shared_keys[6], (2, 1, PAIR_DIM), jnp.float32)], axis=1)
    tri_proj = scaled_normal(shared_keys[7], (2, PAIR_DIM, 4 * TRI_DIM), PAIR_DIM)
    tri_gate = scaled_normal(shared_keys[8], (2, PAIR_DIM, PAIR_DIM), PAIR_DIM)
    tri_xnorm = jnp.concatenate([1.0 + 0.3 * jax.random.normal(shared_keys[9], (2, 1, TRI_DIM), jnp.float32), 0.3 * jax.random.normal(shared_keys[10], (2, 1, TRI_DIM), jnp.float32)], axis=1)
    tri_out = scaled_normal(shared_keys[11], (2, TRI_DIM, PAIR_DIM), TRI_DIM)
    return {"pair_act": pair_act, "pair_mask": pair_mask, "msa_act": msa_act, "opm_norm": opm_norm, "opm_proj": opm_proj, "opm_out": opm_out, "opm_bias": opm_bias, "tri_norm": tri_norm, "tri_proj": tri_proj, "tri_gate": tri_gate, "tri_xnorm": tri_xnorm, "tri_out": tri_out}


def reference(pair_act, pair_mask, msa_act, opm_norm, opm_proj, opm_out, opm_bias, tri_norm, tri_proj, tri_gate, tri_xnorm, tri_out):
    mask_f = pair_mask.astype(jnp.float32)
    pair_zero = pair_act + outer_product_mean(msa_act, opm_norm, opm_proj, opm_out, opm_bias)
    pair_one = triangle_update(pair_zero, mask_f, tri_norm[0], tri_proj[0], tri_gate[0], tri_xnorm[0], tri_out[0], False)
    return triangle_update(pair_one, mask_f, tri_norm[1], tri_proj[1], tri_gate[1], tri_xnorm[1], tri_out[1], True)
```

```python
import functools

import jax
import jax.numpy as jnp
from jax import lax
from jax.experimental import pallas as pl
from jax.experimental.pallas import tpu as pltpu
from jax.sharding import PartitionSpec as P

MESH = pl.DeviceIdType.MESH
LN_EPS = 1e-5
F32 = jnp.float32
BF16 = jnp.bfloat16
N = 128
R = 8
L = 1024
C = 128
JC = 128
NJ = L // JC
SELF = 123
VMEM = pl.BlockSpec(memory_space=pltpu.VMEM)
DMA = pltpu.SemaphoreType.DMA


def dot(lhs, rhs, lhs_dim=1, rhs_dim=0):
    return lax.dot_general(lhs, rhs, (((lhs_dim,), (rhs_dim,)), ((), ())), preferred_element_type=F32)


def sigmoid(v):
    return 0.5 * jnp.tanh(0.5 * v) + 0.5


def layer_norm_rows(v, scale, shift):
    mean = jnp.mean(v, axis=-1, keepdims=True)
    cen = v - mean
    var = jnp.mean(cen * cen, axis=-1, keepdims=True)
    return (cen * lax.rsqrt(var + LN_EPS) * scale + shift).astype(BF16)


def coords(dev):
    return dev // 32, (dev // 8) % 4, (dev // 2) % 4, dev % 2


def index_of(z, y, x, core):
    return ((z * 4 + y) * 4 + x) * 2 + core


def peer_of(me, step):
    z, y, x, core = coords(me)
    return index_of((z + step + 1) % 4, (y + step // 8 + 1) % 4, (x + step // 32 + 1) % 4, (core + step // 4) % 2)


def barrier_all(me):
    sem = pltpu.get_barrier_semaphore()

    def signal(k, carry):
        pl.semaphore_signal(sem, inc=1, device_id={"dap": (me + k) % N}, device_id_type=MESH)
        return carry

    lax.fori_loop(1, N, signal, 0)
    pl.semaphore_wait(sem, N - 1)


def a2a_start(me, src, dst, send_sem, recv_sem):
    pltpu.make_async_copy(src.at[me], dst.at[me], recv_sem).start()

    def step(t, carry):
        peer = peer_of(me, t + (t >= SELF).astype(jnp.int32))
        pltpu.make_async_remote_copy(src.at[peer], dst.at[me], send_sem, recv_sem, device_id={"dap": peer}, device_id_type=MESH).start()
        return carry

    lax.fori_loop(0, N - 1, step, 0)


def a2a_wait(src, dst, send_sem, recv_sem):
    pltpu.make_async_copy(src, dst, recv_sem).wait()
    pltpu.make_async_copy(src.at[pl.ds(0, N - 1)], dst.at[pl.ds(0, N - 1)], send_sem).wait()


def a2a_kernel(n, *refs):
    srcs, dsts, (send_sem, recv_sem) = refs[:n], refs[n:2 * n], refs[2 * n:]
    me = lax.axis_index("dap")
    barrier_all(me)
    for k in range(n):
        a2a_start(me, srcs[k], dsts[k], send_sem.at[k], recv_sem.at[k])
    for k in range(n):
        a2a_wait(srcs[k], dsts[k], send_sem.at[k], recv_sem.at[k])


def all_to_all(cid, *arrays):
    n = len(arrays)
    return pl.pallas_call(
        functools.partial(a2a_kernel, n),
        out_shape=[jax.ShapeDtypeStruct(a.shape, a.dtype) for a in arrays],
        in_specs=[VMEM] * n,
        out_specs=[VMEM] * n,
        scratch_shapes=[DMA((n,)), DMA((n,))],
        compiler_params=pltpu.CompilerParams(collective_id=cid, has_side_effects=True, vmem_limit_bytes=40 << 20),
        name="exchange%d" % cid,
    )(*arrays)


AG_PARTS = ((0, 768, (2, 1, 0)), (768, 768, (1, 0, 2)), (1536, 512, (0, 2, 1)))


def gather_kernel(own, out, send_sem, recv_sem, core_send, core_recv, own_sem):
    me = lax.axis_index("dap")
    pos = coords(me)
    core = pos[3]
    barrier_all(me)
    chip = me // 2
    cp = pltpu.make_async_copy(own, out.at[core, chip], own_sem)
    cp.start()
    cp.wait()

    def moved(p, axis, by):
        q = list(p)
        q[axis] = (q[axis] + by) % 4
        return q

    def chip_of(p):
        return (p[0] * 4 + p[1]) * 4 + p[2]

    for stage in range(3):
        for part, (lo, width, order) in enumerate(AG_PARTS):
            lanes = pl.ds(lo, width)
            if stage > 0:
                blk = out.at[0, pl.ds(0, 3 * 4 ** (stage - 1)), :, lanes]
                pltpu.make_async_copy(blk, blk, recv_sem.at[part, stage - 1]).wait()
            for by in (1, 3, 2):
                to = moved(pos, order[stage], by)
                peer = chip_of(to) * 2 + core

                def send(b, carry):
                    p = list(pos)
                    if stage > 0:
                        p = moved(p, order[0], b % 4)
                    if stage > 1:
                        p = moved(p, order[1], b // 4)
                    blk = out.at[core, chip_of(p), :, lanes]
                    pltpu.make_async_remote_copy(blk, blk, send_sem.at[part, stage], recv_sem.at[part, stage], device_id={"dap": peer}, device_id_type=MESH).start()
                    return carry

                lax.fori_loop(0, 4 ** stage, send, 0)
    for part, (lo, width, order) in enumerate(AG_PARTS):
        lanes = pl.ds(lo, width)
        blk = out.at[0, pl.ds(0, 48), :, lanes]
        pltpu.make_async_copy(blk, blk, recv_sem.at[part, 2]).wait()
        blk = out.at[core, :, :, lanes]
        pltpu.make_async_remote_copy(blk, blk, core_send.at[part], core_recv.at[part], device_id={"dap": chip * 2 + 1 - core}, device_id_type=MESH).start()
    for part, (lo, width, order) in enumerate(AG_PARTS):
        lanes = pl.ds(lo, width)
        for stage in range(3):
            blk = out.at[0, pl.ds(0, 3 * 4 ** stage), :, lanes]
            pltpu.make_async_copy(blk, blk, send_sem.at[part, stage]).wait()
        blk = out.at[0, :, :, lanes]
        pltpu.make_async_copy(blk, blk, core_send.at[part]).wait()
        pltpu.make_async_copy(blk, blk, core_recv.at[part]).wait()


def gather_right(cid, own):
    return pl.pallas_call(
        gather_kernel,
        out_shape=jax.ShapeDtypeStruct((2, N // 2, R, 2048), BF16),
        in_specs=[VMEM],
        out_specs=VMEM,
        scratch_shapes=[DMA((3, 3)), DMA((3, 3)), DMA((3,)), DMA((3,)), DMA],
        compiler_params=pltpu.CompilerParams(collective_id=cid, has_side_effects=True, vmem_limit_bytes=40 << 20),
        name="gather%d" % cid,
    )(own)


def project(y_pair, mask_pair, w_ref, spread_a, spread_b, ip):
    for half, spread in ((0, spread_a), (1, spread_b)):
        lo = half * 2 * C
        act = dot(w_ref[lo:lo + C], y_pair, 1, 1)
        gate = dot(w_ref[lo + C:lo + 2 * C], y_pair, 1, 1)
        vals = mask_pair * sigmoid(gate) * act
        spread[pl.ds(2 * ip, C, stride=R), :] = vals[:, :JC]
        spread[pl.ds(2 * ip + 1, C, stride=R), :] = vals[:, JC:]


def mask_of(mask_ref, ip, cols):
    return jnp.concatenate([mask_ref[2 * ip:2 * ip + 1, cols], mask_ref[2 * ip + 1:2 * ip + 2, cols]], axis=1).astype(F32)


def flush(spread, out_ref, cols):
    out_ref[:, :, cols] = spread[...].reshape(C, R, JC).astype(BF16)


def opm_project_kernel(pair_ref, mask_ref, right_ref, left_ref, wo_ref, bias_ref, norm_ref, w_ref, z_ref, y_ref, a_ref, b_ref, outer, spread_a, spread_b):
    def chunk(jc, carry):
        cols = pl.ds(pl.multiple_of(jc * JC, JC), JC)
        chips = pl.ds(jc * 8, 8)
        for ip in range(R // 2):
            for g in range(8):
                lanes = slice(g * 256, (g + 1) * 256)
                rows = jnp.concatenate([right_ref[0, chips, :, lanes].reshape(8, 1, R, 256), right_ref[1, chips, :, lanes].reshape(8, 1, R, 256)], axis=1).reshape(JC, 256)
                o = (dot(rows, left_ref[ip]) * (1.0 / 64)).astype(BF16)
                outer[0, :, g * C:(g + 1) * C] = o[:, :C]
                outer[1, :, g * C:(g + 1) * C] = o[:, C:]
            ys = []
            for h in range(2):
                z = pair_ref[2 * ip + h, cols, :] + (dot(outer[h], wo_ref[...]) + bias_ref[...])
                z_ref[2 * ip + h, cols, :] = z
                y = layer_norm_rows(z, norm_ref[0:1], norm_ref[1:2])
                y_ref[2 * ip + h, cols, :] = y
                ys.append(y)
            project(jnp.concatenate(ys, axis=0), mask_of(mask_ref, ip, cols), w_ref, spread_a, spread_b, ip)
        flush(spread_a, a_ref, cols)
        flush(spread_b, b_ref, cols)
        return carry

    lax.fori_loop(0, NJ, chunk, 0)


def mix_kernel(incoming, a_ref, b_ref, x_ref):
    right = b_ref[...].reshape(L, L)

    def block(n, carry):
        if incoming:
            left = a_ref[:, :, pl.ds(pl.multiple_of(n * C, C), C)].reshape(L, C)
            x = dot(left, right, 0, 0)
        else:
            left = a_ref[pl.ds(n * 16, 16)].reshape(C, L)
            x = dot(left, right, 1, 1)
        x_ref[pl.ds(n * 16, 16)] = x.reshape(16, R, L).astype(BF16)
        return carry

    lax.fori_loop(0, L // C, block, 0)


def update_kernel(last, *refs):
    if last:
        x_ref, z_in, y_in, xscale, xshift, wout, wgate, z_ref, spread = refs
    else:
        x_ref, z_in, y_in, xscale, xshift, wout, wgate, mask_ref, norm_ref, w_ref, z_ref, y_ref, a_ref, b_ref, spread, spread_a, spread_b = refs

    def chunk(jc, carry):
        cols = pl.ds(pl.multiple_of(jc * JC, JC), JC)
        x = x_ref[:, :, cols].astype(F32)
        mean = jnp.mean(x, axis=0, keepdims=True)
        cen = x - mean
        var = jnp.mean(cen * cen, axis=0, keepdims=True)
        spread[...] = (cen * lax.rsqrt(var + LN_EPS)).reshape(C * R, JC)
        for ip in range(R // 2):
            ys = []
            for h in range(2):
                i = 2 * ip + h
                xn = (spread[pl.ds(i, C, stride=R), :] * xscale[...] + xshift[...]).astype(BF16)
                gate = sigmoid(dot(y_in[i, cols, :], wgate[...]))
                z = z_in[i, cols, :] + gate * dot(xn, wout[...], 0, 0)
                z_ref[i, cols, :] = z
                if not last:
                    y = layer_norm_rows(z, norm_ref[0:1], norm_ref[1:2])
                    y_ref[i, cols, :] = y
                    ys.append(y)
            if not last:
                project(jnp.concatenate(ys, axis=0), mask_of(mask_ref, ip, cols), w_ref, spread_a, spread_b, ip)
        if not last:
            flush(spread_a, a_ref, cols)
            flush(spread_b, b_ref, cols)
        return carry

    lax.fori_loop(0, NJ, chunk, 0)


PAIR = jax.ShapeDtypeStruct((R, L, C), F32)
NORMED = jax.ShapeDtypeStruct((R, L, C), BF16)
CHAN = jax.ShapeDtypeStruct((C, R, L), BF16)
SPREAD = pltpu.VMEM((C * R, JC), F32)
PARAMS = pltpu.CompilerParams(vmem_limit_bytes=56 << 20)


def call(kernel, outs, scratch, *args):
    return pl.pallas_call(kernel, out_shape=outs, in_specs=[VMEM] * len(args), out_specs=[VMEM] * len(outs), scratch_shapes=scratch, compiler_params=PARAMS)(*args)


def opm_operands(msa, opm_norm, opm_proj, opm_out):
    depth = msa.shape[0]
    normed = layer_norm_rows(msa.astype(F32), opm_norm[0], opm_norm[1])
    u = jnp.einsum("srm,mp->srp", normed, opm_proj, preferred_element_type=F32).astype(BF16)
    right = jnp.transpose(u[:, :, 32:], (1, 2, 0)).reshape(R, 32 * depth)
    left = jnp.transpose(u[:, :, :32], (1, 0, 2)).reshape(R // 2, 2, 1, depth, 1, 32)
    eye = jnp.eye(4, dtype=BF16).reshape(1, 1, 4, 1, 4, 1)
    blocks = (left * eye).reshape(R // 2, 2, 4 * depth, 128)
    left_wide = jnp.transpose(blocks, (0, 2, 1, 3)).reshape(R // 2, 4 * depth, 256)
    out_w = jnp.transpose(opm_out.reshape(32, 32, C), (1, 0, 2)).reshape(1024, C)
    return right, left_wide, out_w


def solution(mesh):
    row_spec = P(("data", "dap"), None, None)
    mask_spec = P(("data", "dap"), None)
    msa_spec = P(None, ("data", "dap"), None)
    rep = P()

    def local_program(pair, mask, msa, opm_norm, opm_proj, opm_out, opm_bias, tri_norm, tri_proj, tri_gate, tri_xnorm, tri_out):
        right, left, out_w = opm_operands(msa, opm_norm, opm_proj, opm_out)
        w_t = jnp.swapaxes(tri_proj, 1, 2)
        xn = jnp.broadcast_to(tri_xnorm[:, :, :, None], (2, 2, C, JC))
        right_all = gather_right(0, right)
        z, y, a, b = call(opm_project_kernel, [PAIR, NORMED, CHAN, CHAN], [pltpu.VMEM((2, JC, 1024), BF16), SPREAD, SPREAD],
                          pair, mask, right_all, left, out_w, opm_bias[None], tri_norm[0], w_t[0])
        b, a = all_to_all(1, b, a)
        x, = call(functools.partial(mix_kernel, False), [CHAN], [], a, b)
        x, = all_to_all(2, x)
        z, y, a, b = call(functools.partial(update_kernel, False), [PAIR, NORMED, CHAN, CHAN], [SPREAD, SPREAD, SPREAD],
                          x, z, y, xn[0, 0], xn[0, 1], tri_out[0], tri_gate[0], mask, tri_norm[1], w_t[1])
        b, a = all_to_all(3, b, a)
        x, = call(functools.partial(mix_kernel, True), [CHAN], [], a, b)
        x, = all_to_all(4, x)
        z, = call(functools.partial(update_kernel, True), [PAIR], [SPREAD], x, z, y, xn[1, 0], xn[1, 1], tri_out[1], tri_gate[1])
        return z

    return jax.shard_map(local_program, mesh=mesh, in_specs=(row_spec, mask_spec, msa_spec) + (rep,) * 9, out_specs=row_spec, check_vma=False)
```

```python
import functools

import jax
import jax.numpy as jnp
from jax import lax
from jax.experimental import pallas as pl
from jax.experimental.pallas import tpu as pltpu
from jax.sharding import PartitionSpec as P

MESH = pl.DeviceIdType.MESH
LN_EPS = 1e-5
F32 = jnp.float32
BF16 = jnp.bfloat16
N = 128
R = 8
L = 1024
C = 128
JC = 128
NJ = L // JC
KC = 256
NK = L // KC
VMEM = pl.BlockSpec(memory_space=pltpu.VMEM)
DMA = pltpu.SemaphoreType.DMA


def dot(lhs, rhs, lhs_dim=1, rhs_dim=0):
    return lax.dot_general(lhs, rhs, (((lhs_dim,), (rhs_dim,)), ((), ())), preferred_element_type=F32)


def sigmoid(v):
    return 0.5 * jnp.tanh(0.5 * v) + 0.5


def layer_norm_rows(v, scale, shift):
    mean = jnp.mean(v, axis=-1, keepdims=True)
    cen = v - mean
    var = jnp.mean(cen * cen, axis=-1, keepdims=True)
    return (cen * lax.rsqrt(var + LN_EPS) * scale + shift).astype(BF16)


def coords(dev):
    return dev >> 5, (dev >> 3) & 3, (dev >> 1) & 3, dev & 1


def barrier_all(me):
    sem = pltpu.get_barrier_semaphore()

    def signal(k, carry):
        pl.semaphore_signal(sem, inc=1, device_id={"dap": me ^ k}, device_id_type=MESH)
        return carry

    lax.fori_loop(1, N, signal, 0)
    pl.semaphore_wait(sem, N - 1)


def send_chunk(me, kc, pairs):
    cols = pl.ds(pl.multiple_of(kc * KC, KC), KC)

    def send(peer):
        for src, dst, send_sem, recv_sem in pairs:
            pltpu.make_async_remote_copy(src.at[peer, :, cols], dst.at[me, :, cols], send_sem, recv_sem, device_id={"dap": peer}, device_id_type=MESH).start()

    for src, dst, send_sem, recv_sem in pairs:
        pltpu.make_async_copy(src.at[me, :, cols], dst.at[me, :, cols], recv_sem).start()

    def outer(o, carry):
        base = me ^ (o & 3) * 2 ^ (o >> 2)
        for n in range(1, 16):
            send(base ^ ((n & 3) << 5 | (n >> 2) << 3))
        return carry

    lax.fori_loop(0, 8, outer, 0)

    def plane(o, carry):
        send(me ^ (o & 3) * 2 ^ (o >> 2))
        return carry

    lax.fori_loop(1, 8, plane, 0)


def wait_chunk(buf, kc, recv_sem):
    blk = buf.at[:, :, pl.ds(pl.multiple_of(kc * KC, KC), KC)]
    pltpu.make_async_copy(blk, blk, recv_sem).wait()


def wait_sent(buf, send_sem):
    blk = buf.at[pl.ds(0, N - 1)]
    pltpu.make_async_copy(blk, blk, send_sem).wait()


AG_PARTS = ((0, 768, (2, 1, 0)), (768, 768, (1, 0, 2)), (1536, 512, (0, 2, 1)))


def gather(me, own, out, send_sem, recv_sem, core_send, core_recv, own_sem):
    pos = coords(me)
    core = pos[3]
    chip = me >> 1
    cp = pltpu.make_async_copy(own, out.at[core, chip], own_sem)
    cp.start()
    cp.wait()

    def moved(p, axis, by):
        q = list(p)
        q[axis] = (q[axis] + by) & 3
        return q

    def chip_of(p):
        return (p[0] << 4) | (p[1] << 2) | p[2]

    for stage in range(3):
        for part, (lo, width, order) in enumerate(AG_PARTS):
            lanes = pl.ds(lo, width)
            if stage > 0:
                blk = out.at[0, pl.ds(0, 3 * 4 ** (stage - 1)), :, lanes]
                pltpu.make_async_copy(blk, blk, recv_sem.at[part, stage - 1]).wait()
            for by in (1, 3, 2):
                peer = chip_of(moved(pos, order[stage], by)) * 2 + core

                def send(b, carry):
                    p = list(pos)
                    if stage > 0:
                        p = moved(p, order[0], b & 3)
                    if stage > 1:
                        p = moved(p, order[1], b >> 2)
                    blk = out.at[core, chip_of(p), :, lanes]
                    pltpu.make_async_remote_copy(blk, blk, send_sem.at[part, stage], recv_sem.at[part, stage], device_id={"dap": peer}, device_id_type=MESH).start()
                    return carry

                lax.fori_loop(0, 4 ** stage, send, 0)
    for part, (lo, width, order) in enumerate(AG_PARTS):
        lanes = pl.ds(lo, width)
        blk = out.at[0, pl.ds(0, 48), :, lanes]
        pltpu.make_async_copy(blk, blk, recv_sem.at[part, 2]).wait()
        blk = out.at[core, :, :, lanes]
        pltpu.make_async_remote_copy(blk, blk, core_send.at[part], core_recv.at[part], device_id={"dap": chip * 2 + 1 - core}, device_id_type=MESH).start()
    for part, (lo, width, order) in enumerate(AG_PARTS):
        lanes = pl.ds(lo, width)
        for stage in range(3):
            blk = out.at[0, pl.ds(0, 3 * 4 ** stage), :, lanes]
            pltpu.make_async_copy(blk, blk, send_sem.at[part, stage]).wait()
        blk = out.at[0, :, :, lanes]
        pltpu.make_async_copy(blk, blk, core_send.at[part]).wait()
        pltpu.make_async_copy(blk, blk, core_recv.at[part]).wait()


def project(y_pair, mask_pair, w_ref, half, spread, ip):
    lo = half * 2 * C
    act = dot(w_ref[lo:lo + C], y_pair, 1, 1)
    gate = dot(w_ref[lo + C:lo + 2 * C], y_pair, 1, 1)
    vals = mask_pair * sigmoid(gate) * act
    spread[pl.ds(2 * ip, C, stride=R), :] = vals[:, :JC]
    spread[pl.ds(2 * ip + 1, C, stride=R), :] = vals[:, JC:]


def mask_of(mask_ref, ip, cols):
    return jnp.concatenate([mask_ref[2 * ip:2 * ip + 1, cols], mask_ref[2 * ip + 1:2 * ip + 2, cols]], axis=1).astype(F32)


def flush(spread, out_ref, cols):
    out_ref[:, :, cols] = spread[...].reshape(C, R, JC).astype(BF16)


def columns(kc, sub):
    return pl.ds(pl.multiple_of(kc * KC + sub * JC, JC), JC)


def opm_chunk(kc, sub, pair_ref, mask_ref, right_all, left_ref, wo_ref, bias_ref, norm_ref, w_ref, z_ref, y_ref, a_ref, b_ref, rows, outer, spread_a, spread_b):
    cols = columns(kc, sub)
    chips = pl.ds(kc * (KC // 16) + sub * (JC // 16), JC // 16)
    rows[...] = jnp.concatenate([right_all[core, chips].reshape(JC // 16, 1, R, 2048) for core in range(2)], axis=1).reshape(JC, 2048)
    for ip in range(R // 2):
        for g in range(8):
            o = (dot(rows[:, g * 256:(g + 1) * 256], left_ref[ip]) * (1.0 / 64)).astype(BF16)
            outer[0, :, g * C:(g + 1) * C] = o[:, :C]
            outer[1, :, g * C:(g + 1) * C] = o[:, C:]
        ys = []
        for h in range(2):
            z = pair_ref[2 * ip + h, cols, :] + (dot(outer[h], wo_ref[...]) + bias_ref[...])
            z_ref[2 * ip + h, cols, :] = z
            y = layer_norm_rows(z, norm_ref[0, 0:1], norm_ref[0, 1:2])
            y_ref[2 * ip + h, cols, :] = y
            ys.append(y)
        y_pair = jnp.concatenate(ys, axis=0)
        mask_pair = mask_of(mask_ref, ip, cols)
        project(y_pair, mask_pair, w_ref.at[0], 0, spread_a, ip)
        project(y_pair, mask_pair, w_ref.at[0], 1, spread_b, ip)
    flush(spread_a, a_ref, cols)
    flush(spread_b, b_ref, cols)


def update_chunk(kc, sub, t, x_ref, xnorm, wout, wgate, mask_ref, norm_ref, w_ref, z_ref, y_ref, a_ref, spread, spread_a):
    cols = columns(kc, sub)
    x = x_ref[:, :, cols].astype(F32)
    mean = jnp.mean(x, axis=0, keepdims=True)
    cen = x - mean
    var = jnp.mean(cen * cen, axis=0, keepdims=True)
    spread[...] = (cen * lax.rsqrt(var + LN_EPS)).reshape(C * R, JC)
    for ip in range(R // 2):
        ys = []
        for h in range(2):
            i = 2 * ip + h
            xn = (spread[pl.ds(i, C, stride=R), :] * xnorm[t, 0] + xnorm[t, 1]).astype(BF16)
            gate = sigmoid(dot(y_ref[i, cols, :], wgate[t]))
            z = z_ref[i, cols, :] + gate * dot(xn, wout[t], 0, 0)
            z_ref[i, cols, :] = z
            if t == 0:
                y = layer_norm_rows(z, norm_ref[1, 0:1], norm_ref[1, 1:2])
                y_ref[i, cols, :] = y
                ys.append(y)
        if t == 0:
            project(jnp.concatenate(ys, axis=0), mask_of(mask_ref, ip, cols), w_ref.at[1], 0, spread_a, ip)
    if t == 0:
        flush(spread_a, a_ref, cols)


def right_chunk(kc, sub, mask_ref, w_ref, y_ref, b_ref, spread_b):
    cols = columns(kc, sub)
    for ip in range(R // 2):
        y_pair = jnp.concatenate([y_ref[2 * ip, cols, :], y_ref[2 * ip + 1, cols, :]], axis=0)
        project(y_pair, mask_of(mask_ref, ip, cols), w_ref.at[1], 1, spread_b, ip)
    flush(spread_b, b_ref, cols)


def for_subs(fn):
    def step(sub, carry):
        fn(sub)
        return carry

    lax.fori_loop(0, KC // JC, step, 0)


def for_chunks(fn):
    def step(kc, carry):
        fn(kc)
        return carry

    lax.fori_loop(0, NK, step, 0)


def whole_kernel(pair_ref, mask_ref, own, left_ref, wo_ref, bias_ref, norm_ref, w_ref, xnorm, wout, wgate, z_ref,
                 right_all, y_ref, sent_a, sent_b, got_a, got_b, sent_x, got_x, left_full, right_full, rows, outer, spread, spread_a, spread_b,
                 ag_send, ag_recv, core_send, core_recv, own_sem, send_sem, recv_sem):
    me = lax.axis_index("dap")
    barrier_all(me)
    gather(me, own, right_all, ag_send, ag_recv, core_send, core_recv, own_sem)

    def first(kc):
        for_subs(lambda sub: opm_chunk(kc, sub, pair_ref, mask_ref, right_all, left_ref, wo_ref, bias_ref, norm_ref, w_ref, z_ref, y_ref, sent_a.at[0], sent_b.at[0], rows, outer, spread_a, spread_b))
        send_chunk(me, kc, ((sent_a.at[0], got_a.at[0], send_sem.at[0], recv_sem.at[0, kc]), (sent_b.at[0], got_b.at[0], send_sem.at[1], recv_sem.at[1, kc])))

    for_chunks(first)

    def arrive(kc):
        cols = pl.ds(pl.multiple_of(kc * KC, KC), KC)
        wait_chunk(got_a.at[0], kc, recv_sem.at[0, kc])
        left_full[:, cols] = got_a[0, :, :, cols].reshape(L, KC)
        wait_chunk(got_b.at[0], kc, recv_sem.at[1, kc])
        right_full[:, cols] = got_b[0, :, :, cols].reshape(L, KC)

    for_chunks(arrive)

    def outgoing(kc):
        cols = pl.ds(pl.multiple_of(kc * KC, KC), KC)
        x = dot(left_full[...], right_full[cols, :], 1, 1)
        sent_x[0, :, :, cols] = x.reshape(N, R, KC).astype(BF16)
        send_chunk(me, kc, ((sent_x.at[0], got_x.at[0], send_sem.at[2], recv_sem.at[2, kc]),))

    for_chunks(outgoing)

    def middle(kc):
        wait_chunk(got_x.at[0], kc, recv_sem.at[2, kc])
        for_subs(lambda sub: update_chunk(kc, sub, 0, got_x.at[0], xnorm, wout, wgate, mask_ref, norm_ref, w_ref, z_ref, y_ref, sent_a.at[1], spread, spread_a))
        send_chunk(me, kc, ((sent_a.at[1], got_a.at[1], send_sem.at[3], recv_sem.at[3, kc]),))

    for_chunks(middle)

    def right_side(kc):
        for_subs(lambda sub: right_chunk(kc, sub, mask_ref, w_ref, y_ref, sent_b.at[1], spread_b))
        send_chunk(me, kc, ((sent_b.at[1], got_b.at[1], send_sem.at[4], recv_sem.at[4, kc]),))

    for_chunks(right_side)

    def turn(kc):
        wait_chunk(got_a.at[1], kc, recv_sem.at[3, kc])
        cols = pl.ds(pl.multiple_of(kc * KC, KC), KC)
        left_full[cols, :] = got_a[1, :, :, cols].reshape(L, KC).T

    for_chunks(turn)

    def incoming(kc):
        cols = pl.ds(pl.multiple_of(kc * KC, KC), KC)
        wait_chunk(got_b.at[1], kc, recv_sem.at[4, kc])
        x = dot(left_full[...], got_b[1, :, :, cols].reshape(L, KC), 1, 0)
        sent_x[1, :, :, cols] = x.reshape(N, R, KC).astype(BF16)
        send_chunk(me, kc, ((sent_x.at[1], got_x.at[1], send_sem.at[5], recv_sem.at[5, kc]),))

    for_chunks(incoming)

    def final(kc):
        wait_chunk(got_x.at[1], kc, recv_sem.at[5, kc])
        for_subs(lambda sub: update_chunk(kc, sub, 1, got_x.at[1], xnorm, wout, wgate, None, None, None, z_ref, y_ref, None, spread, None))

    for_chunks(final)
    for n, buf in enumerate((sent_a.at[0], sent_b.at[0], sent_x.at[0], sent_a.at[1], sent_b.at[1], sent_x.at[1])):
        wait_sent(buf, send_sem.at[n])


def whole(*args):
    chan2 = pltpu.VMEM((2, N, R, L), BF16)
    spread = pltpu.VMEM((C * R, JC), F32)
    return pl.pallas_call(
        whole_kernel,
        out_shape=jax.ShapeDtypeStruct((R, L, C), F32),
        in_specs=[VMEM] * len(args),
        out_specs=VMEM,
        scratch_shapes=[
            pltpu.VMEM((2, N // 2, R, 2048), BF16), pltpu.VMEM((R, L, C), BF16),
            chan2, chan2, chan2, chan2, chan2, chan2, pltpu.VMEM((L, L), BF16), pltpu.VMEM((L, L), BF16),
            pltpu.VMEM((JC, 2048), BF16), pltpu.VMEM((2, JC, 1024), BF16), spread, spread, spread,
            DMA((3, 3)), DMA((3, 3)), DMA((3,)), DMA((3,)), DMA, DMA((6,)), DMA((6, NK)),
        ],
        compiler_params=pltpu.CompilerParams(collective_id=0, has_side_effects=True, vmem_limit_bytes=50 << 20),
        name="pair_stack",
    )(*args)


def opm_operands(msa, opm_norm, opm_proj, opm_out):
    depth = msa.shape[0]
    normed = layer_norm_rows(msa.astype(F32), opm_norm[0], opm_norm[1])
    u = jnp.einsum("srm,mp->srp", normed, opm_proj, preferred_element_type=F32).astype(BF16)
    right = jnp.transpose(u[:, :, 32:], (1, 2, 0)).reshape(R, 32 * depth)
    left = jnp.transpose(u[:, :, :32], (1, 0, 2)).reshape(R // 2, 2, 1, depth, 1, 32)
    eye = jnp.eye(4, dtype=BF16).reshape(1, 1, 4, 1, 4, 1)
    blocks = (left * eye).reshape(R // 2, 2, 4 * depth, 128)
    left_wide = jnp.transpose(blocks, (0, 2, 1, 3)).reshape(R // 2, 4 * depth, 256)
    out_w = jnp.transpose(opm_out.reshape(32, 32, C), (1, 0, 2)).reshape(1024, C)
    return right, left_wide, out_w


def solution(mesh):
    row_spec = P(("data", "dap"), None, None)
    mask_spec = P(("data", "dap"), None)
    msa_spec = P(None, ("data", "dap"), None)
    rep = P()

    def local_program(pair, mask, msa, opm_norm, opm_proj, opm_out, opm_bias, tri_norm, tri_proj, tri_gate, tri_xnorm, tri_out):
        right, left, out_w = opm_operands(msa, opm_norm, opm_proj, opm_out)
        w_t = jnp.swapaxes(tri_proj, 1, 2)
        xn = jnp.broadcast_to(tri_xnorm[:, :, :, None], (2, 2, C, JC))
        return whole(pair, mask, right, left, out_w, opm_bias[None], tri_norm, w_t, xn, tri_out, tri_gate)

    return jax.shard_map(local_program, mesh=mesh, in_specs=(row_spec, mask_spec, msa_spec) + (rep,) * 9, out_specs=row_spec, check_vma=False)
```

```python
import functools

import jax
import jax.numpy as jnp
from jax import lax
from jax.experimental import pallas as pl
from jax.experimental.pallas import tpu as pltpu
from jax.sharding import PartitionSpec as P

MESH = pl.DeviceIdType.MESH
LN_EPS = 1e-5
F32 = jnp.float32
BF16 = jnp.bfloat16
N = 128
R = 8
L = 1024
C = 128
JC = 128
NJ = L // JC
KC = 256
NK = L // KC
VMEM = pl.BlockSpec(memory_space=pltpu.VMEM)
DMA = pltpu.SemaphoreType.DMA


def dot(lhs, rhs, lhs_dim=1, rhs_dim=0):
    return lax.dot_general(lhs, rhs, (((lhs_dim,), (rhs_dim,)), ((), ())), preferred_element_type=F32)


def sigmoid(v):
    return 0.5 * jnp.tanh(0.5 * v) + 0.5


def layer_norm_rows(v, scale, shift):
    mean = jnp.mean(v, axis=-1, keepdims=True)
    cen = v - mean
    var = jnp.mean(cen * cen, axis=-1, keepdims=True)
    return (cen * lax.rsqrt(var + LN_EPS) * scale + shift).astype(BF16)


def coords(dev):
    return dev >> 5, (dev >> 3) & 3, (dev >> 1) & 3, dev & 1


def barrier_signal(me):
    sem = pltpu.get_barrier_semaphore()

    def signal(k, carry):
        pl.semaphore_signal(sem, inc=1, device_id={"dap": me ^ k}, device_id_type=MESH)
        return carry

    lax.fori_loop(1, N, signal, 0)


def send_chunk(me, kc, pairs):
    cols = pl.ds(pl.multiple_of(kc * KC, KC), KC)

    def send(peer):
        for src, dst, send_sem, recv_sem in pairs:
            pltpu.make_async_remote_copy(src.at[peer, :, cols], dst.at[me, :, cols], send_sem, recv_sem, device_id={"dap": peer}, device_id_type=MESH).start()

    for src, dst, send_sem, recv_sem in pairs:
        pltpu.make_async_copy(src.at[me, :, cols], dst.at[me, :, cols], recv_sem).start()

    def outer(o, carry):
        base = me ^ (o & 3) * 2 ^ (o >> 2)
        for n in range(1, 16):
            send(base ^ ((n & 3) << 5 | (n >> 2) << 3))
        return carry

    lax.fori_loop(0, 8, outer, 0)

    def plane(o, carry):
        send(me ^ (o & 3) * 2 ^ (o >> 2))
        return carry

    lax.fori_loop(1, 8, plane, 0)


def wait_chunk(buf, kc, recv_sem):
    blk = buf.at[:, :, pl.ds(pl.multiple_of(kc * KC, KC), KC)]
    pltpu.make_async_copy(blk, blk, recv_sem).wait()


def wait_sent(buf, send_sem):
    blk = buf.at[pl.ds(0, N - 1)]
    pltpu.make_async_copy(blk, blk, send_sem).wait()


PARTS = ((0, 768), (768, 768), (1536, 512))
STREAMS = ((0, 2, 1), (1, 1, 1), (2, 2, 1), (2, 0, 1), (0, 1, 4), (1, 2, 4), (2, 1, 4), (1, 0, 4), (2, 2, 3), (0, 0, 16), (1, 2, 12), (2, 1, 12))


def moved(p, axis, by):
    q = list(p)
    q[axis] = (q[axis] + by) & 3
    return q


def chip_of(p):
    return (p[0] << 4) | (p[1] << 2) | p[2]


def stream_block(n, pos, b):
    if n < 4:
        return pos
    if n in (4, 6):
        return moved(pos, 2, b)
    if n in (5, 7):
        return moved(pos, 1, b)
    if n == 8:
        return moved(pos, 0, b + 1)
    if n == 9:
        return moved(moved(pos, 2, b & 3), 1, b >> 2)
    return moved(moved(pos, 1 if n == 10 else 2, b & 3), 0, (b >> 2) + 1)


def gather_send(n, pos, buf, send_sem, recv_sem):
    part, axis, count = STREAMS[n]
    core = pos[3]
    lanes = pl.ds(*PARTS[part])

    def step(b, carry):
        blk = buf.at[core, chip_of(stream_block(n, pos, b)), :, lanes]
        for by in (1, 3, 2):
            peer = chip_of(moved(pos, axis, by)) * 2 + core
            pltpu.make_async_remote_copy(blk, blk, send_sem.at[n], recv_sem.at[n], device_id={"dap": peer}, device_id_type=MESH).start()
        return carry

    lax.fori_loop(0, count, step, 0)


def gather_wait(n, buf, sem):
    part, axis, count = STREAMS[n]
    blk = buf.at[0, pl.ds(0, 3 * count), :, pl.ds(*PARTS[part])]
    pltpu.make_async_copy(blk, blk, sem.at[n]).wait()


def core_send_plane(me, plane, buf, send_sem, recv_sem):
    blk = buf.at[me & 1, pl.ds(pl.multiple_of(plane * 16, 16), 16)]
    pltpu.make_async_remote_copy(blk, blk, send_sem.at[plane], recv_sem.at[plane], device_id={"dap": me ^ 1}, device_id_type=MESH).start()


def core_wait_plane(plane, buf, sem):
    blk = buf.at[0, pl.ds(0, 16)]
    pltpu.make_async_copy(blk, blk, sem.at[plane]).wait()


def own_projection(me, msa_ref, onorm_ref, proj_ref, right_all, spread_a, spread_b):
    depth = msa_ref.shape[0]
    normed = layer_norm_rows(msa_ref[...].astype(F32).reshape(depth * R, 256), onorm_ref[0:1], onorm_ref[1:2])
    wide = jnp.concatenate([proj_ref[:32]] * 4 + [proj_ref[32:]] * 4, axis=0)
    u = dot(normed, wide, 1, 1)
    spread_a[pl.ds(0, depth * R), :] = u[:, :C]
    spread_b[pl.ds(0, depth * R), :] = u[:, C:]
    for r in range(R):
        turned = spread_b[pl.ds(r, depth, stride=R), :].T
        spread_a[pl.ds(depth * R + r, 16, stride=R), :] = jnp.concatenate([turned[0:16], turned[16:32]], axis=1)
    for n in range(16):
        right_all[me & 1, me >> 1, :, n * C:(n + 1) * C] = spread_a[pl.ds(depth * R + n * R, R), :].astype(BF16)


def prepare(oout_ref, w_in, xn_in, left_ref, wo_ref, w_ref, xnorm, spread, spread_a):
    depth = 64
    group = lax.broadcasted_iota(jnp.int32, (depth, C), 1) >> 5
    for r in range(R):
        left = spread_a[pl.ds(r, depth, stride=R), :]
        for n in range(4):
            left_ref[r // 2, n * depth:(n + 1) * depth, (r % 2) * C:(r % 2 + 1) * C] = jnp.where(group == n, left, 0.0).astype(BF16)
    spread[...] = oout_ref[...].astype(F32)
    for n in range(32):
        q = (n % 2) * 16 + n // 2
        wo_ref[n * 32:(n + 1) * 32, :] = spread[pl.ds(q, 32, stride=32), :].astype(BF16)
    for t in range(2):
        w_ref[t] = w_in[t].T
        for k in range(2):
            xnorm[t, k] = jnp.broadcast_to(xn_in[t, k:k + 1], (C, C)).T


def project(y_pair, mask_pair, w_ref, half, spread, ip):
    lo = half * 2 * C
    act = dot(w_ref[lo:lo + C], y_pair, 1, 1)
    gate = dot(w_ref[lo + C:lo + 2 * C], y_pair, 1, 1)
    vals = mask_pair * sigmoid(gate) * act
    spread[pl.ds(2 * ip, C, stride=R), :] = vals[:, :JC]
    spread[pl.ds(2 * ip + 1, C, stride=R), :] = vals[:, JC:]


def mask_of(mask_ref, ip, cols):
    return jnp.concatenate([mask_ref[2 * ip:2 * ip + 1, cols], mask_ref[2 * ip + 1:2 * ip + 2, cols]], axis=1).astype(F32)


def flush(spread, out_ref, cols):
    out_ref[:, :, cols] = spread[...].reshape(C, R, JC).astype(BF16)


def columns(kc, sub):
    return pl.ds(pl.multiple_of(kc * KC + sub * JC, JC), JC)


def opm_chunk(kc, sub, mask_ref, right_all, left_ref, wo_ref, bias_ref, norm_ref, w_ref, z_ref, y_ref, a_ref, b_ref, rows, outer, spread_a, spread_b):
    cols = columns(kc, sub)
    chips = pl.ds(kc * (KC // 16) + sub * (JC // 16), JC // 16)
    rows[...] = jnp.concatenate([right_all[core, chips].reshape(JC // 16, 1, R, 2048) for core in range(2)], axis=1).reshape(JC, 2048)
    for ip in range(R // 2):
        for g in range(8):
            o = (dot(rows[:, g * 256:(g + 1) * 256], left_ref[ip]) * (1.0 / 64)).astype(BF16)
            outer[0, :, g * C:(g + 1) * C] = o[:, :C]
            outer[1, :, g * C:(g + 1) * C] = o[:, C:]
        ys = []
        for h in range(2):
            z = z_ref[2 * ip + h, cols, :] + (dot(outer[h], wo_ref[...]) + bias_ref[...])
            z_ref[2 * ip + h, cols, :] = z
            y = layer_norm_rows(z, norm_ref[0, 0:1], norm_ref[0, 1:2])
            y_ref[2 * ip + h, cols, :] = y
            ys.append(y)
        y_pair = jnp.concatenate(ys, axis=0)
        mask_pair = mask_of(mask_ref, ip, cols)
        project(y_pair, mask_pair, w_ref.at[0], 0, spread_a, ip)
        project(y_pair, mask_pair, w_ref.at[0], 1, spread_b, ip)
    flush(spread_a, a_ref, cols)
    flush(spread_b, b_ref, cols)


def update_chunk(kc, sub, t, x_ref, xnorm, wout, wgate, mask_ref, norm_ref, w_ref, z_ref, y_ref, a_ref, spread, spread_a):
    cols = columns(kc, sub)
    x = x_ref[:, :, cols].astype(F32)
    mean = jnp.mean(x, axis=0, keepdims=True)
    cen = x - mean
    var = jnp.mean(cen * cen, axis=0, keepdims=True)
    spread[...] = (cen * lax.rsqrt(var + LN_EPS)).reshape(C * R, JC)
    for ip in range(R // 2):
        ys = []
        for h in range(2):
            i = 2 * ip + h
            xn = (spread[pl.ds(i, C, stride=R), :] * xnorm[t, 0] + xnorm[t, 1]).astype(BF16)
            gate = sigmoid(dot(y_ref[i, cols, :], wgate[t]))
            z = z_ref[i, cols, :] + gate * dot(xn, wout[t], 0, 0)
            z_ref[i, cols, :] = z
            if t == 0:
                y = layer_norm_rows(z, norm_ref[1, 0:1], norm_ref[1, 1:2])
                y_ref[i, cols, :] = y
                ys.append(y)
        if t == 0:
            project(jnp.concatenate(ys, axis=0), mask_of(mask_ref, ip, cols), w_ref.at[1], 0, spread_a, ip)
    if t == 0:
        flush(spread_a, a_ref, cols)


def right_chunk(kc, sub, mask_ref, w_ref, y_ref, b_ref, spread_b):
    cols = columns(kc, sub)
    for ip in range(R // 2):
        y_pair = jnp.concatenate([y_ref[2 * ip, cols, :], y_ref[2 * ip + 1, cols, :]], axis=0)
        project(y_pair, mask_of(mask_ref, ip, cols), w_ref.at[1], 1, spread_b, ip)
    flush(spread_b, b_ref, cols)


def for_subs(fn):
    def step(sub, carry):
        fn(sub)
        return carry

    lax.fori_loop(0, KC // JC, step, 0)


def for_chunks(fn):
    def step(kc, carry):
        fn(kc)
        return carry

    lax.fori_loop(0, NK, step, 0)


def whole_kernel(*refs):
    sources, (z_ref,), staged, refs = refs[:12], refs[12:13], refs[13:24], refs[24:]
    mask_ref, msa_ref, onorm_ref, proj_ref, oout_ref, bias_ref, norm_ref, w_in, xn_in, wout, wgate = staged
    (left_ref, wo_ref, w_ref, xnorm,
     right_all, y_ref, sent_a, sent_b, got_a, got_b, sent_x, got_x, left_full, right_full, rows, outer, spread, spread_a, spread_b,
     ag_send, ag_recv, core_send, core_recv, in_sem, send_sem, recv_sem) = refs
    me = lax.axis_index("dap")
    pos = coords(me)
    plane = pos[0]
    barrier_signal(me)
    loads = [pltpu.make_async_copy(src, dst, in_sem.at[n]) for n, (src, dst) in enumerate(zip(sources, (z_ref,) + tuple(staged)))]
    for n in (2, 3, 4, 1, 5, 6, 7, 8, 9, 10, 11, 0):
        loads[n].start()
    for n in (2, 3, 4):
        loads[n].wait()
    own_projection(me, msa_ref, onorm_ref, proj_ref, right_all, spread_a, spread_b)
    pl.semaphore_wait(pltpu.get_barrier_semaphore(), N - 1)

    def send(*streams):
        for n in streams:
            gather_send(n, pos, right_all, ag_send, ag_recv)

    def wait(*streams):
        for n in streams:
            gather_wait(n, right_all, ag_recv)

    send(0, 1, 2, 3)
    for n in (1, 5, 6, 7, 8, 9, 10, 11):
        loads[n].wait()
    prepare(oout_ref, w_in, xn_in, left_ref, wo_ref, w_ref, xnorm, spread, spread_a)
    wait(0)
    send(4)
    wait(1)
    send(5)
    wait(2)
    send(6, 7)
    wait(3)
    send(8)
    wait(4)
    send(9)
    wait(5, 6)
    core_send_plane(me, plane, right_all, core_send, core_recv)
    wait(7)
    send(10)
    wait(8)
    send(11)
    loads[0].wait()

    def first(t):
        kc = (plane + t) & 3

        @pl.when(t == 1)
        def _():
            wait(9, 10, 11)
            for by in (1, 2, 3):
                core_send_plane(me, (plane + by) & 3, right_all, core_send, core_recv)

        core_wait_plane(kc, right_all, core_recv)
        for_subs(lambda sub: opm_chunk(kc, sub, mask_ref, right_all, left_ref, wo_ref, bias_ref, norm_ref, w_ref, z_ref, y_ref, sent_a.at[0], sent_b.at[0], rows, outer, spread_a, spread_b))
        send_chunk(me, kc, ((sent_a.at[0], got_a.at[0], send_sem.at[0], recv_sem.at[0, kc]), (sent_b.at[0], got_b.at[0], send_sem.at[1], recv_sem.at[1, kc])))

    for_chunks(first)

    def arrive(kc):
        cols = pl.ds(pl.multiple_of(kc * KC, KC), KC)
        wait_chunk(got_a.at[0], kc, recv_sem.at[0, kc])
        left_full[:, cols] = got_a[0, :, :, cols].reshape(L, KC)
        wait_chunk(got_b.at[0], kc, recv_sem.at[1, kc])
        right_full[:, cols] = got_b[0, :, :, cols].reshape(L, KC)

    for_chunks(arrive)

    def outgoing(kc):
        cols = pl.ds(pl.multiple_of(kc * KC, KC), KC)
        x = dot(left_full[...], right_full[cols, :], 1, 1)
        sent_x[0, :, :, cols] = x.reshape(N, R, KC).astype(BF16)
        send_chunk(me, kc, ((sent_x.at[0], got_x.at[0], send_sem.at[2], recv_sem.at[2, kc]),))

    for_chunks(outgoing)

    def middle(kc):
        wait_chunk(got_x.at[0], kc, recv_sem.at[2, kc])
        for_subs(lambda sub: update_chunk(kc, sub, 0, got_x.at[0], xnorm, wout, wgate, mask_ref, norm_ref, w_ref, z_ref, y_ref, sent_a.at[1], spread, spread_a))
        send_chunk(me, kc, ((sent_a.at[1], got_a.at[1], send_sem.at[3], recv_sem.at[3, kc]),))

    for_chunks(middle)

    def right_side(kc):
        for_subs(lambda sub: right_chunk(kc, sub, mask_ref, w_ref, y_ref, sent_b.at[1], spread_b))
        send_chunk(me, kc, ((sent_b.at[1], got_b.at[1], send_sem.at[4], recv_sem.at[4, kc]),))

    for_chunks(right_side)

    def turn(kc):
        wait_chunk(got_a.at[1], kc, recv_sem.at[3, kc])
        cols = pl.ds(pl.multiple_of(kc * KC, KC), KC)
        left_full[cols, :] = got_a[1, :, :, cols].reshape(L, KC).T

    for_chunks(turn)

    def incoming(kc):
        cols = pl.ds(pl.multiple_of(kc * KC, KC), KC)
        wait_chunk(got_b.at[1], kc, recv_sem.at[4, kc])
        x = dot(left_full[...], got_b[1, :, :, cols].reshape(L, KC), 1, 0)
        sent_x[1, :, :, cols] = x.reshape(N, R, KC).astype(BF16)
        send_chunk(me, kc, ((sent_x.at[1], got_x.at[1], send_sem.at[5], recv_sem.at[5, kc]),))

    for_chunks(incoming)

    def final(kc):
        wait_chunk(got_x.at[1], kc, recv_sem.at[5, kc])
        for_subs(lambda sub: update_chunk(kc, sub, 1, got_x.at[1], xnorm, wout, wgate, None, None, None, z_ref, y_ref, None, spread, None))

    for_chunks(final)
    for n, buf in enumerate((sent_a.at[0], sent_b.at[0], sent_x.at[0], sent_a.at[1], sent_b.at[1], sent_x.at[1])):
        wait_sent(buf, send_sem.at[n])
    for n in range(len(STREAMS)):
        gather_wait(n, right_all, ag_send)
    for n in range(4):
        core_wait_plane(n, right_all, core_send)


def whole(*args):
    chan2 = pltpu.VMEM((2, N, R, L), BF16)
    spread = pltpu.VMEM((C * R, JC), F32)
    return pl.pallas_call(
        whole_kernel,
        out_shape=jax.ShapeDtypeStruct((R, L, C), F32),
        in_specs=[pl.BlockSpec(memory_space=pltpu.HBM)] * len(args),
        out_specs=VMEM,
        scratch_shapes=[pltpu.VMEM(v.shape, v.dtype) for v in args[1:]] + [
            pltpu.VMEM((R // 2, 256, 256), BF16), pltpu.VMEM((1024, C), BF16), pltpu.VMEM((2, 4 * C, C), BF16), pltpu.VMEM((2, 2, C, C), F32),
            pltpu.VMEM((2, N // 2, R, 2048), BF16), pltpu.VMEM((R, L, C), BF16),
            chan2, chan2, chan2, chan2, chan2, chan2, pltpu.VMEM((L, L), BF16), pltpu.VMEM((L, L), BF16),
            pltpu.VMEM((JC, 2048), BF16), pltpu.VMEM((2, JC, 1024), BF16), spread, spread, spread,
            DMA((12,)), DMA((12,)), DMA((4,)), DMA((4,)), DMA((12,)), DMA((6,)), DMA((6, NK)),
        ],
        compiler_params=pltpu.CompilerParams(collective_id=0, has_side_effects=True, vmem_limit_bytes=46 << 20),
        name="pair_stack",
    )(*args)


def solution(mesh):
    row_spec = P(("data", "dap"), None, None)
    mask_spec = P(("data", "dap"), None)
    msa_spec = P(None, ("data", "dap"), None)
    rep = P()

    def local_program(pair, mask, msa, opm_norm, opm_proj, opm_out, opm_bias, tri_norm, tri_proj, tri_gate, tri_xnorm, tri_out):
        return whole(pair, mask, msa, opm_norm, opm_proj.T, opm_out, opm_bias[None], tri_norm, tri_proj, tri_xnorm, tri_out, tri_gate)

    return jax.shard_map(local_program, mesh=mesh, in_specs=(row_spec, mask_spec, msa_spec) + (rep,) * 9, out_specs=row_spec, check_vma=False)
```

```python
import functools

import jax
import jax.numpy as jnp
from jax import lax
from jax.experimental import pallas as pl
from jax.experimental.pallas import tpu as pltpu
from jax.sharding import PartitionSpec as P

MESH = pl.DeviceIdType.MESH
LN_EPS = 1e-5
F32 = jnp.float32
BF16 = jnp.bfloat16
N = 128
R = 8
L = 1024
C = 128
JC = 128
NJ = L // JC
KC = 256
NK = L // KC
VMEM = pl.BlockSpec(memory_space=pltpu.VMEM)
DMA = pltpu.SemaphoreType.DMA


def dot(lhs, rhs, lhs_dim=1, rhs_dim=0):
    return lax.dot_general(lhs, rhs, (((lhs_dim,), (rhs_dim,)), ((), ())), preferred_element_type=F32)


def sigmoid(v):
    return 0.5 * jnp.tanh(0.5 * v) + 0.5


def layer_norm_rows(v, scale, shift):
    mean = jnp.mean(v, axis=-1, keepdims=True)
    cen = v - mean
    var = jnp.mean(cen * cen, axis=-1, keepdims=True)
    return (cen * lax.rsqrt(var + LN_EPS) * scale + shift).astype(BF16)


def coords(dev):
    return dev >> 5, (dev >> 3) & 3, (dev >> 1) & 3, dev & 1


def barrier_signal(me):
    sem = pltpu.get_barrier_semaphore()

    def signal(k, carry):
        pl.semaphore_signal(sem, inc=1, device_id={"dap": me ^ k}, device_id_type=MESH)
        return carry

    lax.fori_loop(1, N, signal, 0)


def send_chunk(me, kc, pairs):
    cols = pl.ds(pl.multiple_of(kc * KC, KC), KC)

    def send(peer):
        for src, dst, send_sem, recv_sem in pairs:
            pltpu.make_async_remote_copy(src.at[peer, :, cols], dst.at[me, :, cols], send_sem, recv_sem, device_id={"dap": peer}, device_id_type=MESH).start()

    for src, dst, send_sem, recv_sem in pairs:
        pltpu.make_async_copy(src.at[me, :, cols], dst.at[me, :, cols], recv_sem).start()

    def outer(o, carry):
        base = me ^ (o & 3) * 2 ^ (o >> 2)
        for n in range(1, 16):
            send(base ^ ((n & 3) << 5 | (n >> 2) << 3))
        return carry

    lax.fori_loop(0, 8, outer, 0)

    def plane(o, carry):
        send(me ^ (o & 3) * 2 ^ (o >> 2))
        return carry

    lax.fori_loop(1, 8, plane, 0)


def wait_chunk(buf, kc, recv_sem):
    blk = buf.at[:, :, pl.ds(pl.multiple_of(kc * KC, KC), KC)]
    pltpu.make_async_copy(blk, blk, recv_sem).wait()


def wait_sent(buf, send_sem):
    blk = buf.at[pl.ds(0, N - 1)]
    pltpu.make_async_copy(blk, blk, send_sem).wait()


PARTS = ((0, 768), (768, 768), (1536, 512))
STREAMS = ((0, 2, 1), (1, 1, 1), (2, 2, 1), (2, 0, 1), (0, 1, 4), (1, 2, 4), (2, 1, 4), (1, 0, 4), (2, 2, 3), (0, 0, 16), (1, 2, 12), (2, 1, 12))


def moved(p, axis, by):
    q = list(p)
    q[axis] = (q[axis] + by) & 3
    return q


def chip_of(p):
    return (p[0] << 4) | (p[1] << 2) | p[2]


def stream_block(n, pos, b):
    if n < 4:
        return pos
    if n in (4, 6):
        return moved(pos, 2, b)
    if n in (5, 7):
        return moved(pos, 1, b)
    if n == 8:
        return moved(pos, 0, b + 1)
    if n == 9:
        return moved(moved(pos, 2, b & 3), 1, b >> 2)
    return moved(moved(pos, 1 if n == 10 else 2, b & 3), 0, (b >> 2) + 1)


def gather_send(n, pos, buf, send_sem, recv_sem):
    part, axis, count = STREAMS[n]
    core = pos[3]
    lanes = pl.ds(*PARTS[part])

    def step(b, carry):
        blk = buf.at[core, chip_of(stream_block(n, pos, b)), :, lanes]
        for by in (1, 3, 2):
            peer = chip_of(moved(pos, axis, by)) * 2 + core
            pltpu.make_async_remote_copy(blk, blk, send_sem.at[n], recv_sem.at[n], device_id={"dap": peer}, device_id_type=MESH).start()
        return carry

    lax.fori_loop(0, count, step, 0)


def gather_wait(n, buf, sem):
    part, axis, count = STREAMS[n]
    blk = buf.at[0, pl.ds(0, 3 * count), :, pl.ds(*PARTS[part])]
    pltpu.make_async_copy(blk, blk, sem.at[n]).wait()


def core_send_plane(me, plane, buf, send_sem, recv_sem):
    blk = buf.at[me & 1, pl.ds(pl.multiple_of(plane * 16, 16), 16)]
    pltpu.make_async_remote_copy(blk, blk, send_sem.at[plane], recv_sem.at[plane], device_id={"dap": me ^ 1}, device_id_type=MESH).start()


def core_wait_plane(plane, buf, sem):
    blk = buf.at[0, pl.ds(0, 16)]
    pltpu.make_async_copy(blk, blk, sem.at[plane]).wait()


def own_projection(me, msa_ref, onorm_ref, proj_ref, right_all, spread_a, spread_b):
    depth = msa_ref.shape[0]
    normed = layer_norm_rows(msa_ref[...].astype(F32).reshape(depth * R, 256), onorm_ref[0:1], onorm_ref[1:2])
    wide = jnp.concatenate([proj_ref[:32]] * 4 + [proj_ref[32:]] * 4, axis=0)
    u = dot(normed, wide, 1, 1)
    spread_a[pl.ds(0, depth * R), :] = u[:, :C]
    spread_b[pl.ds(0, depth * R), :] = u[:, C:]
    for r in range(R):
        turned = spread_b[pl.ds(r, depth, stride=R), :].T
        spread_a[pl.ds(depth * R + r, 16, stride=R), :] = jnp.concatenate([turned[0:16], turned[16:32]], axis=1)
    for n in range(16):
        right_all[me & 1, me >> 1, :, n * C:(n + 1) * C] = spread_a[pl.ds(depth * R + n * R, R), :].astype(BF16)


def prepare(oout_ref, w_in, xn_in, left_ref, wo_ref, w_ref, xnorm, spread, spread_a):
    depth = 64
    group = lax.broadcasted_iota(jnp.int32, (depth, C), 1) >> 5
    for r in range(R):
        left = spread_a[pl.ds(r, depth, stride=R), :]
        for n in range(4):
            left_ref[r // 2, n * depth:(n + 1) * depth, (r % 2) * C:(r % 2 + 1) * C] = jnp.where(group == n, left, 0.0).astype(BF16)
    spread[...] = oout_ref[...].astype(F32)
    for n in range(32):
        q = (n % 2) * 16 + n // 2
        wo_ref[n * 32:(n + 1) * 32, :] = spread[pl.ds(q, 32, stride=32), :].astype(BF16)
    for t in range(2):
        w_ref[t] = w_in[t].T
        for k in range(2):
            xnorm[t, k] = jnp.broadcast_to(xn_in[t, k:k + 1], (C, C)).T


def project(y_pair, mask_pair, w_ref, half, spread, ip):
    lo = half * 2 * C
    act = dot(w_ref[lo:lo + C], y_pair, 1, 1)
    gate = dot(w_ref[lo + C:lo + 2 * C], y_pair, 1, 1)
    vals = mask_pair * sigmoid(gate) * act
    spread[pl.ds(2 * ip, C, stride=R), :] = vals[:, :JC]
    spread[pl.ds(2 * ip + 1, C, stride=R), :] = vals[:, JC:]


def mask_of(mask_ref, ip, cols):
    return jnp.concatenate([mask_ref[2 * ip:2 * ip + 1, cols], mask_ref[2 * ip + 1:2 * ip + 2, cols]], axis=1).astype(F32)


def flush(spread, out_ref, cols):
    out_ref[:, :, cols] = spread[...].reshape(C, R, JC).astype(BF16)


def columns(kc, sub):
    return pl.ds(pl.multiple_of(kc * KC + sub * JC, JC), JC)


def opm_chunk(kc, sub, mask_ref, right_all, left_ref, wo_ref, bias_ref, norm_ref, w_ref, z_ref, y_ref, a_ref, b_ref, rows, outer, spread_a, spread_b):
    cols = columns(kc, sub)
    chips = pl.ds(kc * (KC // 16) + sub * (JC // 16), JC // 16)
    got = jnp.concatenate([right_all[core, chips].reshape(JC // 16, 1, R, 2048) for core in range(2)], axis=1).reshape(JC, 2048)
    for g in range(8):
        rows[g * JC:(g + 1) * JC, :] = got[:, g * 256:(g + 1) * 256]
    for ip in range(R // 2):
        o = (dot(rows[...], left_ref[ip]) * (1.0 / 64)).astype(BF16)
        for h in range(2):
            for g in range(8):
                outer[pl.ds((2 * ip + h) * JC, JC), g * C:(g + 1) * C] = o[g * JC:(g + 1) * JC, h * C:(h + 1) * C]
    opm = dot(outer[...], wo_ref[...]) + bias_ref[...]
    for ip in range(R // 2):
        ys = []
        for h in range(2):
            z = z_ref[2 * ip + h, cols, :] + opm[(2 * ip + h) * JC:(2 * ip + h + 1) * JC]
            z_ref[2 * ip + h, cols, :] = z
            y = layer_norm_rows(z, norm_ref[0, 0:1], norm_ref[0, 1:2])
            y_ref[2 * ip + h, cols, :] = y
            ys.append(y)
        y_pair = jnp.concatenate(ys, axis=0)
        mask_pair = mask_of(mask_ref, ip, cols)
        project(y_pair, mask_pair, w_ref.at[0], 0, spread_a, ip)
        project(y_pair, mask_pair, w_ref.at[0], 1, spread_b, ip)
    flush(spread_a, a_ref, cols)
    flush(spread_b, b_ref, cols)


def update_chunk(kc, sub, t, x_ref, xnorm, wout, wgate, mask_ref, norm_ref, w_ref, z_ref, y_ref, a_ref, spread, spread_a):
    cols = columns(kc, sub)
    x = x_ref[:, :, cols].astype(F32)
    mean = jnp.mean(x, axis=0, keepdims=True)
    cen = x - mean
    var = jnp.mean(cen * cen, axis=0, keepdims=True)
    spread[...] = (cen * lax.rsqrt(var + LN_EPS)).reshape(C * R, JC)
    for ip in range(R // 2):
        ys = []
        for h in range(2):
            i = 2 * ip + h
            xn = (spread[pl.ds(i, C, stride=R), :] * xnorm[t, 0] + xnorm[t, 1]).astype(BF16)
            gate = sigmoid(dot(y_ref[i, cols, :], wgate[t]))
            z = z_ref[i, cols, :] + gate * dot(xn, wout[t], 0, 0)
            z_ref[i, cols, :] = z
            if t == 0:
                y = layer_norm_rows(z, norm_ref[1, 0:1], norm_ref[1, 1:2])
                y_ref[i, cols, :] = y
                ys.append(y)
        if t == 0:
            project(jnp.concatenate(ys, axis=0), mask_of(mask_ref, ip, cols), w_ref.at[1], 0, spread_a, ip)
    if t == 0:
        flush(spread_a, a_ref, cols)


def right_chunk(kc, sub, mask_ref, w_ref, y_ref, b_ref, spread_b):
    cols = columns(kc, sub)
    for ip in range(R // 2):
        y_pair = jnp.concatenate([y_ref[2 * ip, cols, :], y_ref[2 * ip + 1, cols, :]], axis=0)
        project(y_pair, mask_of(mask_ref, ip, cols), w_ref.at[1], 1, spread_b, ip)
    flush(spread_b, b_ref, cols)


def for_subs(fn):
    def step(sub, carry):
        fn(sub)
        return carry

    lax.fori_loop(0, KC // JC, step, 0)


def for_chunks(fn):
    def step(kc, carry):
        fn(kc)
        return carry

    lax.fori_loop(0, NK, step, 0)


def whole_kernel(*refs):
    sources, (z_ref,), staged, refs = refs[:12], refs[12:13], refs[13:24], refs[24:]
    mask_ref, msa_ref, onorm_ref, proj_ref, oout_ref, bias_ref, norm_ref, w_in, xn_in, wout, wgate = staged
    (left_ref, wo_ref, w_ref, xnorm,
     right_all, y_ref, sent_a, sent_b, got_a, got_b, sent_x, got_x, left_full, right_full, rows, outer, spread, spread_a, spread_b,
     ag_send, ag_recv, core_send, core_recv, in_sem, send_sem, recv_sem) = refs
    me = lax.axis_index("dap")
    pos = coords(me)
    plane = pos[0]
    barrier_signal(me)
    loads = [pltpu.make_async_copy(src, dst, in_sem.at[n]) for n, (src, dst) in enumerate(zip(sources, (z_ref,) + tuple(staged)))]
    for n in (2, 3, 4, 1, 5, 6, 7, 8, 9, 10, 11, 0):
        loads[n].start()
    for n in (2, 3, 4):
        loads[n].wait()
    own_projection(me, msa_ref, onorm_ref, proj_ref, right_all, spread_a, spread_b)
    pl.semaphore_wait(pltpu.get_barrier_semaphore(), N - 1)

    def send(*streams):
        for n in streams:
            gather_send(n, pos, right_all, ag_send, ag_recv)

    def wait(*streams):
        for n in streams:
            gather_wait(n, right_all, ag_recv)

    send(0, 1, 2, 3)
    for n in (1, 5, 6, 7, 8, 9, 10, 11):
        loads[n].wait()
    prepare(oout_ref, w_in, xn_in, left_ref, wo_ref, w_ref, xnorm, spread, spread_a)
    wait(0)
    send(4)
    wait(1)
    send(5)
    wait(2)
    send(6, 7)
    wait(3)
    send(8)
    wait(4)
    send(9)
    wait(5, 6)
    core_send_plane(me, plane, right_all, core_send, core_recv)
    wait(7)
    send(10)
    wait(8)
    send(11)
    loads[0].wait()

    def first(t):
        kc = (plane + t) & 3

        @pl.when(t == 1)
        def _():
            wait(9, 10, 11)
            for by in (1, 2, 3):
                core_send_plane(me, (plane + by) & 3, right_all, core_send, core_recv)

        core_wait_plane(kc, right_all, core_recv)
        for_subs(lambda sub: opm_chunk(kc, sub, mask_ref, right_all, left_ref, wo_ref, bias_ref, norm_ref, w_ref, z_ref, y_ref, sent_a.at[0], sent_b.at[0], rows, outer, spread_a, spread_b))
        send_chunk(me, kc, ((sent_a.at[0], got_a.at[0], send_sem.at[0], recv_sem.at[0, kc]), (sent_b.at[0], got_b.at[0], send_sem.at[1], recv_sem.at[1, kc])))

    for_chunks(first)

    def arrive(kc):
        cols = pl.ds(pl.multiple_of(kc * KC, KC), KC)
        wait_chunk(got_a.at[0], kc, recv_sem.at[0, kc])
        left_full[:, cols] = got_a[0, :, :, cols].reshape(L, KC)
        wait_chunk(got_b.at[0], kc, recv_sem.at[1, kc])
        right_full[:, cols] = got_b[0, :, :, cols].reshape(L, KC)

    for_chunks(arrive)

    def outgoing(kc):
        cols = pl.ds(pl.multiple_of(kc * KC, KC), KC)
        x = dot(left_full[...], right_full[cols, :], 1, 1)
        sent_x[0, :, :, cols] = x.reshape(N, R, KC).astype(BF16)
        send_chunk(me, kc, ((sent_x.at[0], got_x.at[0], send_sem.at[2], recv_sem.at[2, kc]),))

    for_chunks(outgoing)

    def middle(kc):
        wait_chunk(got_x.at[0], kc, recv_sem.at[2, kc])
        for_subs(lambda sub: update_chunk(kc, sub, 0, got_x.at[0], xnorm, wout, wgate, mask_ref, norm_ref, w_ref, z_ref, y_ref, sent_a.at[1], spread, spread_a))
        send_chunk(me, kc, ((sent_a.at[1], got_a.at[1], send_sem.at[3], recv_sem.at[3, kc]),))

    for_chunks(middle)

    def right_side(kc):
        for_subs(lambda sub: right_chunk(kc, sub, mask_ref, w_ref, y_ref, sent_b.at[1], spread_b))
        send_chunk(me, kc, ((sent_b.at[1], got_b.at[1], send_sem.at[4], recv_sem.at[4, kc]),))

    for_chunks(right_side)

    def turn(kc):
        wait_chunk(got_a.at[1], kc, recv_sem.at[3, kc])
        cols = pl.ds(pl.multiple_of(kc * KC, KC), KC)
        left_full[cols, :] = got_a[1, :, :, cols].reshape(L, KC).T

    for_chunks(turn)

    def incoming(kc):
        cols = pl.ds(pl.multiple_of(kc * KC, KC), KC)
        wait_chunk(got_b.at[1], kc, recv_sem.at[4, kc])
        x = dot(left_full[...], got_b[1, :, :, cols].reshape(L, KC), 1, 0)
        sent_x[1, :, :, cols] = x.reshape(N, R, KC).astype(BF16)
        send_chunk(me, kc, ((sent_x.at[1], got_x.at[1], send_sem.at[5], recv_sem.at[5, kc]),))

    for_chunks(incoming)

    def final(kc):
        wait_chunk(got_x.at[1], kc, recv_sem.at[5, kc])
        for_subs(lambda sub: update_chunk(kc, sub, 1, got_x.at[1], xnorm, wout, wgate, None, None, None, z_ref, y_ref, None, spread, None))

    for_chunks(final)
    for n, buf in enumerate((sent_a.at[0], sent_b.at[0], sent_x.at[0], sent_a.at[1], sent_b.at[1], sent_x.at[1])):
        wait_sent(buf, send_sem.at[n])
    for n in range(len(STREAMS)):
        gather_wait(n, right_all, ag_send)
    for n in range(4):
        core_wait_plane(n, right_all, core_send)


def whole(*args):
    chan2 = pltpu.VMEM((2, N, R, L), BF16)
    spread = pltpu.VMEM((C * R, JC), F32)
    return pl.pallas_call(
        whole_kernel,
        out_shape=jax.ShapeDtypeStruct((R, L, C), F32),
        in_specs=[pl.BlockSpec(memory_space=pltpu.HBM)] * len(args),
        out_specs=VMEM,
        scratch_shapes=[pltpu.VMEM(v.shape, v.dtype) for v in args[1:]] + [
            pltpu.VMEM((R // 2, 256, 256), BF16), pltpu.VMEM((1024, C), BF16), pltpu.VMEM((2, 4 * C, C), BF16), pltpu.VMEM((2, 2, C, C), F32),
            pltpu.VMEM((2, N // 2, R, 2048), BF16), pltpu.VMEM((R, L, C), BF16),
            chan2, chan2, chan2, chan2, chan2, chan2, pltpu.VMEM((L, L), BF16), pltpu.VMEM((L, L), BF16),
            pltpu.VMEM((8 * JC, 256), BF16), pltpu.VMEM((R * JC, 1024), BF16), spread, spread, spread,
            DMA((12,)), DMA((12,)), DMA((4,)), DMA((4,)), DMA((12,)), DMA((6,)), DMA((6, NK)),
        ],
        compiler_params=pltpu.CompilerParams(collective_id=0, has_side_effects=True, vmem_limit_bytes=46 << 20),
        name="pair_stack",
    )(*[pltpu.with_memory_space_constraint(v, pltpu.HBM) for v in args])


def solution(mesh):
    row_spec = P(("data", "dap"), None, None)
    mask_spec = P(("data", "dap"), None)
    msa_spec = P(None, ("data", "dap"), None)
    rep = P()

    def local_program(pair, mask, msa, opm_norm, opm_proj, opm_out, opm_bias, tri_norm, tri_proj, tri_gate, tri_xnorm, tri_out):
        return whole(pair, mask, msa, opm_norm, opm_proj.T, opm_out, opm_bias[None], tri_norm, tri_proj, tri_xnorm, tri_out, tri_gate)

    return jax.shard_map(local_program, mesh=mesh, in_specs=(row_spec, mask_spec, msa_spec) + (rep,) * 9, out_specs=row_spec, check_vma=False)
```

```python
import functools

import jax
import jax.numpy as jnp
from jax import lax
from jax.experimental import pallas as pl
from jax.experimental.pallas import tpu as pltpu
from jax.sharding import PartitionSpec as P

MESH = pl.DeviceIdType.MESH
LN_EPS = 1e-5
F32 = jnp.float32
BF16 = jnp.bfloat16
N = 128
R = 8
L = 1024
C = 128
JC = 128
NJ = L // JC
KC = 256
NK = L // KC
VMEM = pl.BlockSpec(memory_space=pltpu.VMEM)
DMA = pltpu.SemaphoreType.DMA


def dot(lhs, rhs, lhs_dim=1, rhs_dim=0):
    return lax.dot_general(lhs, rhs, (((lhs_dim,), (rhs_dim,)), ((), ())), preferred_element_type=F32)


def sigmoid(v):
    return 0.5 * jnp.tanh(0.5 * v) + 0.5


def layer_norm_rows(v, scale, shift):
    mean = jnp.mean(v, axis=-1, keepdims=True)
    cen = v - mean
    var = jnp.mean(cen * cen, axis=-1, keepdims=True)
    return (cen * lax.rsqrt(var + LN_EPS) * scale + shift).astype(BF16)


def coords(dev):
    return dev >> 5, (dev >> 3) & 3, (dev >> 1) & 3, dev & 1


def barrier_signal(me):
    sem = pltpu.get_barrier_semaphore()

    def signal(k, carry):
        pl.semaphore_signal(sem, inc=1, device_id={"dap": me ^ k}, device_id_type=MESH)
        return carry

    lax.fori_loop(1, N, signal, 0)


def send_chunk(me, kc, pairs):
    cols = pl.ds(pl.multiple_of(kc * KC, KC), KC)

    def send(peer):
        for src, dst, send_sem, recv_sem in pairs:
            pltpu.make_async_remote_copy(src.at[peer, :, cols], dst.at[me, :, cols], send_sem, recv_sem, device_id={"dap": peer}, device_id_type=MESH).start()

    for src, dst, send_sem, recv_sem in pairs:
        pltpu.make_async_copy(src.at[me, :, cols], dst.at[me, :, cols], recv_sem).start()

    def outer(o, carry):
        base = me ^ (o & 3) * 2 ^ (o >> 2)
        for n in range(1, 16):
            z = n & 3
            send(base ^ (z << 5 | (z ^ n >> 2) << 3 | (0, 2, 3, 1)[z] << 1))
        return carry

    lax.fori_loop(0, 8, outer, 0)

    def plane(o, carry):
        send(me ^ (o & 3) * 2 ^ (o >> 2))
        return carry

    lax.fori_loop(1, 8, plane, 0)


def wait_chunk(buf, kc, recv_sem):
    blk = buf.at[:, :, pl.ds(pl.multiple_of(kc * KC, KC), KC)]
    pltpu.make_async_copy(blk, blk, recv_sem).wait()


def wait_sent(buf, send_sem):
    blk = buf.at[pl.ds(0, N - 1)]
    pltpu.make_async_copy(blk, blk, send_sem).wait()


PARTS = ((0, 768), (768, 768), (1536, 512))
STREAMS = ((0, 2, 1), (1, 1, 1), (2, 2, 1), (2, 0, 1), (0, 1, 4), (1, 2, 4), (2, 1, 4), (1, 0, 4), (2, 2, 3), (0, 0, 16), (1, 2, 12), (2, 1, 12))


def moved(p, axis, by):
    q = list(p)
    q[axis] = (q[axis] + by) & 3
    return q


def chip_of(p):
    return (p[0] << 4) | (p[1] << 2) | p[2]


def stream_block(n, pos, b):
    if n < 4:
        return pos
    if n in (4, 6):
        return moved(pos, 2, b)
    if n in (5, 7):
        return moved(pos, 1, b)
    if n == 8:
        return moved(pos, 0, b + 1)
    if n == 9:
        return moved(moved(pos, 2, b & 3), 1, b >> 2)
    return moved(moved(pos, 1 if n == 10 else 2, b & 3), 0, (b >> 2) + 1)


def gather_send(n, pos, buf, send_sem, recv_sem):
    part, axis, count = STREAMS[n]
    core = pos[3]
    lanes = pl.ds(*PARTS[part])

    def step(b, carry):
        blk = buf.at[core, chip_of(stream_block(n, pos, b)), :, lanes]
        for by in (1, 3, 2):
            peer = chip_of(moved(pos, axis, by)) * 2 + core
            pltpu.make_async_remote_copy(blk, blk, send_sem.at[n], recv_sem.at[n], device_id={"dap": peer}, device_id_type=MESH).start()
        return carry

    lax.fori_loop(0, count, step, 0)


def gather_wait(n, buf, sem):
    part, axis, count = STREAMS[n]
    blk = buf.at[0, pl.ds(0, 3 * count), :, pl.ds(*PARTS[part])]
    pltpu.make_async_copy(blk, blk, sem.at[n]).wait()


def core_send_plane(me, plane, buf, send_sem, recv_sem):
    blk = buf.at[me & 1, pl.ds(pl.multiple_of(plane * 16, 16), 16)]
    pltpu.make_async_remote_copy(blk, blk, send_sem.at[plane], recv_sem.at[plane], device_id={"dap": me ^ 1}, device_id_type=MESH).start()


def core_wait_plane(plane, buf, sem):
    blk = buf.at[0, pl.ds(0, 16)]
    pltpu.make_async_copy(blk, blk, sem.at[plane]).wait()


def own_projection(me, msa_ref, onorm_ref, proj_ref, right_all, spread_a, spread_b):
    depth = msa_ref.shape[0]
    normed = layer_norm_rows(msa_ref[...].astype(F32).reshape(depth * R, 256), onorm_ref[0:1], onorm_ref[1:2])
    wide = jnp.concatenate([proj_ref[:32]] * 4 + [proj_ref[32:]] * 4, axis=0)
    u = dot(normed, wide, 1, 1)
    spread_a[pl.ds(0, depth * R), :] = u[:, :C]
    spread_b[pl.ds(0, depth * R), :] = u[:, C:]
    for r in range(R):
        turned = spread_b[pl.ds(r, depth, stride=R), :].T
        spread_a[pl.ds(depth * R + r, 16, stride=R), :] = jnp.concatenate([turned[0:16], turned[16:32]], axis=1)
    for n in range(16):
        right_all[me & 1, me >> 1, :, n * C:(n + 1) * C] = spread_a[pl.ds(depth * R + n * R, R), :].astype(BF16)


def prepare(oout_ref, w_in, xn_in, left_ref, wo_ref, w_ref, xnorm, spread, spread_a):
    depth = 64
    group = lax.broadcasted_iota(jnp.int32, (depth, C), 1) >> 5
    for r in range(R):
        left = spread_a[pl.ds(r, depth, stride=R), :]
        for n in range(4):
            left_ref[r // 2, n * depth:(n + 1) * depth, (r % 2) * C:(r % 2 + 1) * C] = jnp.where(group == n, left, 0.0).astype(BF16)
    spread[...] = oout_ref[...].astype(F32)
    for n in range(32):
        q = (n % 2) * 16 + n // 2
        wo_ref[n * 32:(n + 1) * 32, :] = spread[pl.ds(q, 32, stride=32), :].astype(BF16)
    for t in range(2):
        w_ref[t] = w_in[t].T
        for k in range(2):
            xnorm[t, k] = jnp.broadcast_to(xn_in[t, k:k + 1], (C, C)).T


def project(y_pair, mask_pair, w_ref, half, spread, ip):
    lo = half * 2 * C
    act = dot(w_ref[lo:lo + C], y_pair, 1, 1)
    gate = dot(w_ref[lo + C:lo + 2 * C], y_pair, 1, 1)
    vals = mask_pair * sigmoid(gate) * act
    spread[pl.ds(2 * ip, C, stride=R), :] = vals[:, :JC]
    spread[pl.ds(2 * ip + 1, C, stride=R), :] = vals[:, JC:]


def mask_of(mask_ref, ip, cols):
    return jnp.concatenate([mask_ref[2 * ip:2 * ip + 1, cols], mask_ref[2 * ip + 1:2 * ip + 2, cols]], axis=1).astype(F32)


def flush(spread, out_ref, cols):
    out_ref[:, :, cols] = spread[...].reshape(C, R, JC).astype(BF16)


def columns(kc, sub):
    return pl.ds(pl.multiple_of(kc * KC + sub * JC, JC), JC)


def opm_chunk(kc, sub, mask_ref, right_all, left_ref, wo_ref, bias_ref, norm_ref, w_ref, z_ref, y_ref, a_ref, b_ref, rows, outer, spread_a, spread_b):
    cols = columns(kc, sub)
    chips = pl.ds(kc * (KC // 16) + sub * (JC // 16), JC // 16)
    got = jnp.concatenate([right_all[core, chips].reshape(JC // 16, 1, R, 2048) for core in range(2)], axis=1).reshape(JC, 2048)
    for g in range(8):
        rows[g * JC:(g + 1) * JC, :] = got[:, g * 256:(g + 1) * 256]
    for ip in range(R // 2):
        o = (dot(rows[...], left_ref[ip]) * (1.0 / 64)).astype(BF16)
        for h in range(2):
            for g in range(8):
                outer[pl.ds((2 * ip + h) * JC, JC), g * C:(g + 1) * C] = o[g * JC:(g + 1) * JC, h * C:(h + 1) * C]
    opm = dot(outer[...], wo_ref[...]) + bias_ref[...]
    for ip in range(R // 2):
        ys = []
        for h in range(2):
            z = z_ref[2 * ip + h, cols, :] + opm[(2 * ip + h) * JC:(2 * ip + h + 1) * JC]
            z_ref[2 * ip + h, cols, :] = z
            y = layer_norm_rows(z, norm_ref[0, 0:1], norm_ref[0, 1:2])
            y_ref[2 * ip + h, cols, :] = y
            ys.append(y)
        y_pair = jnp.concatenate(ys, axis=0)
        mask_pair = mask_of(mask_ref, ip, cols)
        project(y_pair, mask_pair, w_ref.at[0], 0, spread_a, ip)
        project(y_pair, mask_pair, w_ref.at[0], 1, spread_b, ip)
    flush(spread_a, a_ref, cols)
    flush(spread_b, b_ref, cols)


def update_chunk(kc, sub, t, x_ref, xnorm, wout, wgate, mask_ref, norm_ref, w_ref, z_ref, y_ref, a_ref, spread, spread_a):
    cols = columns(kc, sub)
    x = x_ref[:, :, cols].astype(F32)
    mean = jnp.mean(x, axis=0, keepdims=True)
    cen = x - mean
    var = jnp.mean(cen * cen, axis=0, keepdims=True)
    spread[...] = (cen * lax.rsqrt(var + LN_EPS)).reshape(C * R, JC)
    for ip in range(R // 2):
        ys = []
        for h in range(2):
            i = 2 * ip + h
            xn = (spread[pl.ds(i, C, stride=R), :] * xnorm[t, 0] + xnorm[t, 1]).astype(BF16)
            gate = sigmoid(dot(y_ref[i, cols, :], wgate[t]))
            z = z_ref[i, cols, :] + gate * dot(xn, wout[t], 0, 0)
            z_ref[i, cols, :] = z
            if t == 0:
                y = layer_norm_rows(z, norm_ref[1, 0:1], norm_ref[1, 1:2])
                y_ref[i, cols, :] = y
                ys.append(y)
        if t == 0:
            project(jnp.concatenate(ys, axis=0), mask_of(mask_ref, ip, cols), w_ref.at[1], 0, spread_a, ip)
    if t == 0:
        flush(spread_a, a_ref, cols)


def right_chunk(kc, sub, mask_ref, w_ref, y_ref, b_ref, spread_b):
    cols = columns(kc, sub)
    for ip in range(R // 2):
        y_pair = jnp.concatenate([y_ref[2 * ip, cols, :], y_ref[2 * ip + 1, cols, :]], axis=0)
        project(y_pair, mask_of(mask_ref, ip, cols), w_ref.at[1], 1, spread_b, ip)
    flush(spread_b, b_ref, cols)


def for_subs(fn):
    def step(sub, carry):
        fn(sub)
        return carry

    lax.fori_loop(0, KC // JC, step, 0)


def for_chunks(fn):
    def step(kc, carry):
        fn(kc)
        return carry

    lax.fori_loop(0, NK, step, 0)


def whole_kernel(*refs):
    sources, (z_ref,), staged, refs = refs[:12], refs[12:13], refs[13:24], refs[24:]
    mask_ref, msa_ref, onorm_ref, proj_ref, oout_ref, bias_ref, norm_ref, w_in, xn_in, wout, wgate = staged
    (left_ref, wo_ref, w_ref, xnorm,
     right_all, y_ref, sent_a, sent_b, got_a, got_b, sent_x, got_x, left_full, right_full, rows, outer, spread, spread_a, spread_b,
     ag_send, ag_recv, core_send, core_recv, in_sem, send_sem, recv_sem) = refs
    me = lax.axis_index("dap")
    pos = coords(me)
    plane = pos[0]
    barrier_signal(me)
    loads = [pltpu.make_async_copy(src, dst, in_sem.at[n]) for n, (src, dst) in enumerate(zip(sources, (z_ref,) + tuple(staged)))]
    for n in (2, 3, 4, 1, 5, 6, 7, 8, 9, 10, 11, 0):
        loads[n].start()
    for n in (2, 3, 4):
        loads[n].wait()
    own_projection(me, msa_ref, onorm_ref, proj_ref, right_all, spread_a, spread_b)
    pl.semaphore_wait(pltpu.get_barrier_semaphore(), N - 1)

    def send(*streams):
        for n in streams:
            gather_send(n, pos, right_all, ag_send, ag_recv)

    def wait(*streams):
        for n in streams:
            gather_wait(n, right_all, ag_recv)

    send(0, 1, 2, 3)
    for n in (1, 5, 6, 7, 8, 9, 10, 11):
        loads[n].wait()
    prepare(oout_ref, w_in, xn_in, left_ref, wo_ref, w_ref, xnorm, spread, spread_a)
    wait(0)
    send(4)
    wait(1)
    send(5)
    wait(2)
    send(6, 7)
    wait(3)
    send(8)
    wait(4)
    send(9)
    wait(5, 6)
    core_send_plane(me, plane, right_all, core_send, core_recv)
    wait(7)
    send(10)
    wait(8)
    send(11)
    loads[0].wait()

    def first(t):
        kc = (plane + t) & 3

        @pl.when(t == 1)
        def _():
            wait(9, 10, 11)
            for by in (1, 2, 3):
                core_send_plane(me, (plane + by) & 3, right_all, core_send, core_recv)

        core_wait_plane(kc, right_all, core_recv)
        for_subs(lambda sub: opm_chunk(kc, sub, mask_ref, right_all, left_ref, wo_ref, bias_ref, norm_ref, w_ref, z_ref, y_ref, sent_a.at[0], sent_b.at[0], rows, outer, spread_a, spread_b))
        send_chunk(me, kc, ((sent_a.at[0], got_a.at[0], send_sem.at[0], recv_sem.at[0, kc]), (sent_b.at[0], got_b.at[0], send_sem.at[1], recv_sem.at[1, kc])))

    for_chunks(first)

    def arrive(kc):
        cols = pl.ds(pl.multiple_of(kc * KC, KC), KC)
        wait_chunk(got_a.at[0], kc, recv_sem.at[0, kc])
        left_full[:, cols] = got_a[0, :, :, cols].reshape(L, KC)
        wait_chunk(got_b.at[0], kc, recv_sem.at[1, kc])
        right_full[:, cols] = got_b[0, :, :, cols].reshape(L, KC)

    for_chunks(arrive)

    def outgoing(kc):
        cols = pl.ds(pl.multiple_of(kc * KC, KC), KC)
        x = dot(left_full[...], right_full[cols, :], 1, 1)
        sent_x[0, :, :, cols] = x.reshape(N, R, KC).astype(BF16)
        send_chunk(me, kc, ((sent_x.at[0], got_x.at[0], send_sem.at[2], recv_sem.at[2, kc]),))

    for_chunks(outgoing)

    def middle(kc):
        wait_chunk(got_x.at[0], kc, recv_sem.at[2, kc])
        for_subs(lambda sub: update_chunk(kc, sub, 0, got_x.at[0], xnorm, wout, wgate, mask_ref, norm_ref, w_ref, z_ref, y_ref, sent_a.at[1], spread, spread_a))
        send_chunk(me, kc, ((sent_a.at[1], got_a.at[1], send_sem.at[3], recv_sem.at[3, kc]),))

    for_chunks(middle)

    def right_side(kc):
        for_subs(lambda sub: right_chunk(kc, sub, mask_ref, w_ref, y_ref, sent_b.at[1], spread_b))
        send_chunk(me, kc, ((sent_b.at[1], got_b.at[1], send_sem.at[4], recv_sem.at[4, kc]),))

    for_chunks(right_side)

    def turn(kc):
        wait_chunk(got_a.at[1], kc, recv_sem.at[3, kc])
        cols = pl.ds(pl.multiple_of(kc * KC, KC), KC)
        left_full[cols, :] = got_a[1, :, :, cols].reshape(L, KC).T

    for_chunks(turn)

    def incoming(kc):
        cols = pl.ds(pl.multiple_of(kc * KC, KC), KC)
        wait_chunk(got_b.at[1], kc, recv_sem.at[4, kc])
        x = dot(left_full[...], got_b[1, :, :, cols].reshape(L, KC), 1, 0)
        sent_x[1, :, :, cols] = x.reshape(N, R, KC).astype(BF16)
        send_chunk(me, kc, ((sent_x.at[1], got_x.at[1], send_sem.at[5], recv_sem.at[5, kc]),))

    for_chunks(incoming)

    def final(kc):
        wait_chunk(got_x.at[1], kc, recv_sem.at[5, kc])
        for_subs(lambda sub: update_chunk(kc, sub, 1, got_x.at[1], xnorm, wout, wgate, None, None, None, z_ref, y_ref, None, spread, None))

    for_chunks(final)
    for n, buf in enumerate((sent_a.at[0], sent_b.at[0], sent_x.at[0], sent_a.at[1], sent_b.at[1], sent_x.at[1])):
        wait_sent(buf, send_sem.at[n])
    for n in range(len(STREAMS)):
        gather_wait(n, right_all, ag_send)
    for n in range(4):
        core_wait_plane(n, right_all, core_send)


def whole(*args):
    chan2 = pltpu.VMEM((2, N, R, L), BF16)
    spread = pltpu.VMEM((C * R, JC), F32)
    return pl.pallas_call(
        whole_kernel,
        out_shape=jax.ShapeDtypeStruct((R, L, C), F32),
        in_specs=[pl.BlockSpec(memory_space=pltpu.HBM)] * len(args),
        out_specs=VMEM,
        scratch_shapes=[pltpu.VMEM(v.shape, v.dtype) for v in args[1:]] + [
            pltpu.VMEM((R // 2, 256, 256), BF16), pltpu.VMEM((1024, C), BF16), pltpu.VMEM((2, 4 * C, C), BF16), pltpu.VMEM((2, 2, C, C), F32),
            pltpu.VMEM((2, N // 2, R, 2048), BF16), pltpu.VMEM((R, L, C), BF16),
            chan2, chan2, chan2, chan2, chan2, chan2, pltpu.VMEM((L, L), BF16), pltpu.VMEM((L, L), BF16),
            pltpu.VMEM((8 * JC, 256), BF16), pltpu.VMEM((R * JC, 1024), BF16), spread, spread, spread,
            DMA((12,)), DMA((12,)), DMA((4,)), DMA((4,)), DMA((12,)), DMA((6,)), DMA((6, NK)),
        ],
        compiler_params=pltpu.CompilerParams(collective_id=0, has_side_effects=True, vmem_limit_bytes=46 << 20),
        name="pair_stack",
    )(*[pltpu.with_memory_space_constraint(v, pltpu.HBM) for v in args])


def solution(mesh):
    row_spec = P(("data", "dap"), None, None)
    mask_spec = P(("data", "dap"), None)
    msa_spec = P(None, ("data", "dap"), None)
    rep = P()

    def local_program(pair, mask, msa, opm_norm, opm_proj, opm_out, opm_bias, tri_norm, tri_proj, tri_gate, tri_xnorm, tri_out):
        return whole(pair, mask, msa, opm_norm, opm_proj.T, opm_out, opm_bias[None], tri_norm, tri_proj, tri_xnorm, tri_out, tri_gate)

    return jax.shard_map(local_program, mesh=mesh, in_specs=(row_spec, mask_spec, msa_spec) + (rep,) * 9, out_specs=row_spec, check_vma=False)
```
